128 devices in a mesh: dp: 1, tp: 2 (over core), cp: 64 (over z, y, x).
Axes of the slice: x: 4, y: 4, z: 4, core: 2. Of those that a mesh axis runs over, the one named last changes fastest.
Arguments:
- tokens_in: bfloat16 [16384, 1536], P(('dp', 'cp', 'tp'))
- grad_out: bfloat16 [16384, 1536], P(('dp', 'cp', 'tp'))
- w_query: bfloat16 [1536, 1536], P(None, 'tp')
- w_key: bfloat16 [1536, 256], P(None, 'tp')
- w_value: bfloat16 [1536, 256], P(None, 'tp')
- w_out: bfloat16 [1536, 1536], P('tp')
Outputs:
- output 1: bfloat16 [16384, 1536], P(('dp', 'cp', 'tp'))
- output 2: bfloat16 [16384, 1536], P(('dp', 'cp', 'tp'))
All inputs are finite; a program needn't handle non-finite values.
Results may differ from the reference program's by a relative error of at most 0.00950505.
Values are sent between devices in bfloat16 or wider.
A program may use at most 1 GiB of HBM per device.

```python
import math
import jax
import jax.numpy as jnp
from jax import lax

D = 1536
HQ = 12
HKV = 2
HEAD = 128
CP = 64
SEQ = 16384

GROUP_SIZE = HQ // HKV
SEQ_LOC = SEQ // CP
PIECE = SEQ_LOC // 2
ROW_BLOCK = 2 ** max(3, min(7, int(math.log2(max(1, 2 ** 22 // (SEQ * HQ))))))


def setup_inputs(seed: int = 0, part: int = 0) -> dict:
    base_key = jax.random.key(seed)
    data_key, weight_key = jax.random.split(base_key)
    part_key = jax.random.fold_in(data_key, part)
    key_x, key_dy = jax.random.split(part_key)
    key_q, key_k, key_v, key_o = jax.random.split(weight_key, 4)
    query_gain = math.sqrt(0.5 * math.log(SEQ))
    tokens_in = jax.random.normal(key_x, (SEQ, D), jnp.float32).astype(jnp.bfloat16)
    grad_out = jax.random.normal(key_dy, (SEQ, D), jnp.float32).astype(jnp.bfloat16)
    w_query = (jax.random.normal(key_q, (D, HQ * HEAD), jnp.float32) * (query_gain / math.sqrt(D))).astype(jnp.bfloat16)
    w_key = (jax.random.normal(key_k, (D, HKV * HEAD), jnp.float32) / math.sqrt(D)).astype(jnp.bfloat16)
    w_value = (jax.random.normal(key_v, (D, HKV * HEAD), jnp.float32) / math.sqrt(D)).astype(jnp.bfloat16)
    w_out = (jax.random.normal(key_o, (HQ * HEAD, D), jnp.float32) / math.sqrt(HQ * HEAD)).astype(jnp.bfloat16)
    return dict(tokens_in=tokens_in, grad_out=grad_out, w_query=w_query, w_key=w_key, w_value=w_value, w_out=w_out)


def fold_positions():
    row_ids = jnp.arange(SEQ, dtype=jnp.int32)
    shard_idx = row_ids // SEQ_LOC
    within = row_ids % SEQ_LOC
    piece_id = jnp.where(within < PIECE, shard_idx, 2 * CP - 1 - shard_idx)
    return piece_id * PIECE + within % PIECE


def reference(tokens_in, grad_out, w_query, w_key, w_value, w_out):
    score_scale = HEAD ** -0.5
    positions = fold_positions()
    queries = jnp.dot(tokens_in, w_query, preferred_element_type=jnp.float32).astype(jnp.bfloat16).reshape(SEQ, HKV, GROUP_SIZE, HEAD)
    keys_all = jnp.dot(tokens_in, w_key, preferred_element_type=jnp.float32).astype(jnp.bfloat16).reshape(SEQ, HKV, HEAD)
    values_all = jnp.dot(tokens_in, w_value, preferred_element_type=jnp.float32).astype(jnp.bfloat16).reshape(SEQ, HKV, HEAD)
    d_out = jnp.dot(grad_out, w_out.T, preferred_element_type=jnp.float32).astype(jnp.bfloat16).reshape(SEQ, HKV, GROUP_SIZE, HEAD)
    keys_f32 = keys_all.astype(jnp.float32)
    values_f32 = values_all.astype(jnp.float32)
    block_count = SEQ // ROW_BLOCK

    def block_step(acc_pair, blk_in):
        dk_acc, dv_acc = acc_pair
        q_blk, do_blk, pos_blk = blk_in
        query_f32 = q_blk.astype(jnp.float32)
        dout_f32 = do_blk.astype(jnp.float32)
        scores = jnp.einsum('qhgd,khd->hgqk', query_f32, keys_f32) * score_scale
        allowed = pos_blk[:, None] >= positions[None, :]
        scores = jnp.where(allowed, scores, -jnp.inf)
        log_norm = jax.nn.logsumexp(scores, axis=-1, keepdims=True)
        prob_f32 = jnp.exp(scores - log_norm).astype(jnp.bfloat16).astype(jnp.float32)
        out_blk = jnp.einsum('hgqk,khd->qhgd', prob_f32, values_f32).astype(jnp.bfloat16)
        row_delta = jnp.sum(dout_f32 * out_blk.astype(jnp.float32), axis=-1)
        d_prob = jnp.einsum('qhgd,khd->hgqk', dout_f32, values_f32)
        dscore_f32 = (prob_f32 * (d_prob - jnp.transpose(row_delta, (1, 2, 0))[..., None])).astype(jnp.bfloat16).astype(jnp.float32)
        dq_blk = (jnp.einsum('hgqk,khd->qhgd', dscore_f32, keys_f32) * score_scale).astype(jnp.bfloat16)
        dk_acc = dk_acc + jnp.einsum('hgqk,qhgd->khd', dscore_f32, query_f32) * score_scale
        dv_acc = dv_acc + jnp.einsum('hgqk,qhgd->khd', prob_f32, dout_f32)
        return (dk_acc, dv_acc), (out_blk, dq_blk)

    blk_inputs = (queries.reshape(block_count, ROW_BLOCK, HKV, GROUP_SIZE, HEAD), d_out.reshape(block_count, ROW_BLOCK, HKV, GROUP_SIZE, HEAD), positions.reshape(block_count, ROW_BLOCK))
    zeros_kv = jnp.zeros((SEQ, HKV, HEAD), jnp.float32)
    (dk_sum, dv_sum), (out_blocks, dq_blocks) = lax.scan(block_step, (zeros_kv, zeros_kv), blk_inputs)
    attn_out = out_blocks.reshape(SEQ, HQ * HEAD)
    d_query = dq_blocks.reshape(SEQ, HQ * HEAD)
    layer_out = jnp.dot(attn_out, w_out, preferred_element_type=jnp.float32).astype(jnp.bfloat16)
    grad_in = (jnp.dot(d_query, w_query.T, preferred_element_type=jnp.float32)
               + jnp.dot(dk_sum.astype(jnp.bfloat16).reshape(SEQ, HKV * HEAD), w_key.T, preferred_element_type=jnp.float32)
               + jnp.dot(dv_sum.astype(jnp.bfloat16).reshape(SEQ, HKV * HEAD), w_value.T, preferred_element_type=jnp.float32)).astype(jnp.bfloat16)
    return layer_out, grad_in
```

```python
import functools
import math

import jax
import jax.numpy as jnp
from jax import lax
from jax.experimental import pallas as pl
from jax.experimental.pallas import tpu as pltpu
from jax.sharding import PartitionSpec as P

HEAD_DIM = 128
PIECE = 128
SIDE = 4
LOG2E = math.log2(math.e)
LOWEST = float(jnp.finfo(jnp.float32).min)
MESH = pl.DeviceIdType.MESH
BF = jnp.bfloat16
F32 = jnp.float32

THIRDS = ((0, 176), (176, 160), (336, 176))
AG_HALF = (96, 80, 96)
RS_HALF = (88, 80, 88)
ORDERS = ((2, 1, 0), (1, 0, 2), (0, 2, 1))
STRIDE = (16, 4, 1)
MAX_ROWS = 176


def dot(a, b):
    return lax.dot_general(a, b, (((1,), (0,)), ((), ())), preferred_element_type=F32)


def dot_ta(a, b):
    return lax.dot_general(a, b, (((0,), (0,)), ((), ())), preferred_element_type=F32)


def kernel(groups, qt_ref, q_ref, dot_ref, do_ref, kv_loc, o_out, dq_out, dkv_out,
           kv, dkv, m_ref, l_ref, acc, dqt, delta, ra0, ra1, ra2, sa0, sa1, sa2,
           local_sem, ag_send, ag_recv, rs_send, rs_recv):
    rank = lax.axis_index('cp')
    me = (rank // 16, lax.rem(rank // 4, 4), lax.rem(rank, 4))
    lanes = groups * PIECE
    width = groups * PIECE

    def coord(dim, off):
        return lax.rem(me[dim] + (off + SIDE), SIDE)

    def device(dim, off):
        return {'cp': rank + STRIDE[dim] * (coord(dim, off) - me[dim])}

    def part(ref, phase, third, q, rows, gathered):
        order = ORDERS[third]
        idx = [None, None, None]
        for p, dim in enumerate(order):
            if p == phase:
                idx[dim] = q
            elif (p < phase) == gathered:
                idx[dim] = slice(None)
            else:
                idx[dim] = me[dim]
        return ref.at[idx[0], idx[1], idx[2], pl.ds(rows[0], rows[1])]

    barrier = pltpu.get_barrier_semaphore()
    for dim in range(3):
        for off in (1, -1):
            pl.semaphore_signal(barrier, inc=1, device_id=device(dim, off), device_id_type=MESH)
    own = pltpu.make_async_copy(kv_loc, kv.at[me[0], me[1], me[2]], local_sem)
    own.start()
    pl.semaphore_wait(barrier, 6)
    own.wait()

    sends = []

    def push(src, dst, send, recv, dim, off):
        copy = pltpu.make_async_remote_copy(src_ref=src, dst_ref=dst, send_sem=send, recv_sem=recv,
                                            device_id=device(dim, off), device_id_type=MESH)
        copy.start()
        sends.append(copy)

    def landed(ref, sem):
        pltpu.make_async_copy(ref, ref, sem).wait()

    def ag_copy(phase, third, kind, q, rows):
        dim = ORDERS[third][phase]
        ref = part(kv, phase, third, q, rows, True)
        push(ref, ref, ag_send.at[third, phase, kind], ag_recv.at[third, phase, kind], dim, 1 if kind % 2 == 0 else -1)

    for phase in range(3):
        for third in range(3):
            dim = ORDERS[third][phase]
            start, size = THIRDS[third]
            for kind in (0, 1):
                ag_copy(phase, third, kind, me[dim], (start, size))
        for third in range(3):
            dim = ORDERS[third][phase]
            start, size = THIRDS[third]
            half = AG_HALF[third]
            halves = ((start, half), (start + half, size - half))
            for kind in (0, 1):
                q = coord(dim, -1 if kind == 0 else 1)
                landed(part(kv, phase, third, q, (start, size), True), ag_recv.at[third, phase, kind])
                ag_copy(phase, third, 2 + kind, q, halves[kind])
        for third in range(3):
            dim = ORDERS[third][phase]
            start, size = THIRDS[third]
            half = AG_HALF[third]
            halves = ((start, half), (start + half, size - half))
            for kind in (0, 1):
                landed(part(kv, phase, third, coord(dim, 2), halves[kind], True), ag_recv.at[third, phase, 2 + kind])

    scale = HEAD_DIM ** -0.5
    c = scale * LOG2E

    def block(j):
        return j // 16, lax.rem(j // 4, 4), lax.rem(j, 4)

    def lane_mask(keys):
        krow = lax.broadcasted_iota(jnp.int32, (keys, width), 0)
        qrow = lax.rem(lax.broadcasted_iota(jnp.int32, (keys, width), 1), PIECE)
        return krow - (keys - PIECE) <= qrow

    def fwd_tile(j, keys, half, masked):
        jz, jy, jx = block(j)
        k = kv[jz, jy, jx, 0:keys, :]
        v = kv[jz, jy, jx, 256:256 + keys, :]
        ql = pl.ds(half * width, width)
        s = dot(k, qt_ref[:, ql])
        if masked:
            s = jnp.where(lane_mask(keys), s, LOWEST)
        m_old = m_ref[:, ql]
        m_new = jnp.maximum(m_old, jnp.max(s, axis=0, keepdims=True))
        alpha = jnp.exp2((m_old - m_new) * c)
        p = jnp.exp2((s - m_new) * c)
        m_ref[:, ql] = m_new
        l_ref[:, ql] = l_ref[:, ql] * alpha + jnp.sum(p, axis=0, keepdims=True)
        acc[:, ql] = acc[:, ql] * alpha + dot_ta(v, p.astype(BF))

    m_ref[...] = jnp.full(m_ref.shape, LOWEST, F32)
    l_ref[...] = jnp.zeros(l_ref.shape, F32)
    acc[...] = jnp.zeros(acc.shape, F32)
    fwd_tile(rank, 128, 0, True)
    fwd_tile(rank, 256, 1, True)

    def fwd_low(j, carry):
        fwd_tile(j, 128, 0, False)
        fwd_tile(j, 128, 1, False)
        return carry

    def fwd_high(j, carry):
        fwd_tile(j, 256, 1, False)
        return carry

    lax.fori_loop(0, rank, fwd_low, 0)
    lax.fori_loop(rank + 1, 64, fwd_high, 0)

    l = l_ref[...]
    o = (acc[...] * (1.0 / l)).astype(BF)
    o_out[...] = o
    delta[...] = jnp.sum(dot_ref[...].astype(F32) * o.astype(F32), axis=0, keepdims=True)
    m_ref[...] = m_ref[...] * c + jnp.log(l) * LOG2E
    dqt[...] = jnp.zeros(dqt.shape, F32)

    def bwd_tile(j, keys, half, masked):
        jz, jy, jx = block(j)
        k = kv[jz, jy, jx, 0:keys, :]
        v = kv[jz, jy, jx, 256:256 + keys, :]
        ql = pl.ds(half * width, width)
        s = dot(k, qt_ref[:, ql])
        p = jnp.exp2(s * c - m_ref[:, ql])
        if masked:
            p = jnp.where(lane_mask(keys), p, 0.0)
        pb = p.astype(BF)
        dp = dot(v, dot_ref[:, ql])
        ds = (pb.astype(F32) * (dp - delta[:, ql])).astype(BF)
        dqt[:, ql] += dot_ta(k, ds)
        return dot(ds, q_ref[ql, :]) * scale, dot(pb, do_ref[ql, :])

    zero = jnp.zeros((PIECE, HEAD_DIM), F32)

    def store(j, keys, dk, dv):
        jz, jy, jx = block(j)
        dkv[jz, jy, jx, 0:keys, :] = dk
        dkv[jz, jy, jx, 256:256 + keys, :] = dv
        if keys == 128:
            dkv[jz, jy, jx, 128:256, :] = zero
            dkv[jz, jy, jx, 384:512, :] = zero

    def bwd_low(j, carry):
        dk0, dv0 = bwd_tile(j, 128, 0, False)
        dk1, dv1 = bwd_tile(j, 128, 1, False)
        store(j, 128, dk0 + dk1, dv0 + dv1)
        return carry

    def bwd_high(j, carry):
        store(j, 256, *bwd_tile(j, 256, 1, False))
        return carry

    store(rank, 256, *bwd_tile(rank, 256, 1, True))
    dk0, dv0 = bwd_tile(rank, 128, 0, True)
    dkv[me[0], me[1], me[2], 0:128, :] += dk0
    dkv[me[0], me[1], me[2], 256:384, :] += dv0
    lax.fori_loop(0, rank, bwd_low, 0)
    lax.fori_loop(rank + 1, 64, bwd_high, 0)
    dq_out[...] = (dqt[...] * scale).astype(BF)

    ra = (ra0, ra1, ra2)
    sa = (sa0, sa1, sa2)

    def rs_split(third):
        start, size = THIRDS[third]
        half = RS_HALF[third]
        return (start, half), (start + half, size - half)

    def add_rows(phase, third, q, rows, sources):
        order = ORDERS[third]
        free = [order[p] for p in range(phase + 1, 3)]

        def one(u, carry):
            idx = {d: me[d] for d in order[:phase]}
            idx[order[phase]] = q
            sub = {}
            for n, d in enumerate(sorted(free)):
                sub[d] = lax.rem(u // SIDE ** (len(free) - 1 - n), SIDE)
            idx.update(sub)
            lead = tuple(sub[d] for d in sorted(free))
            total = dkv[idx[0], idx[1], idx[2], rows[0]:rows[0] + rows[1], :]
            for ref, offset in sources:
                total = total + ref[(*lead, slice(offset, offset + rows[1]), slice(None))]
            dkv[idx[0], idx[1], idx[2], rows[0]:rows[0] + rows[1], :] = total
            return carry

        lax.fori_loop(0, SIDE ** len(free), one, 0)

    for phase in range(3):
        lead = (slice(None),) * (2 - phase)

        def stage(third, sign, offset, size):
            return sa[phase].at[(third, sign, *lead, pl.ds(offset, size))]

        def relay(third, sign, size):
            return ra[phase].at[(third, sign, *lead, pl.ds(0, size))]

        def rs_push(third, kind, q, rows, dst):
            dim = ORDERS[third][phase]
            push(part(dkv, phase, third, q, rows, False), dst, rs_send.at[third, phase, kind],
                 rs_recv.at[third, phase, kind], dim, 1 if kind % 2 == 0 else -1)

        for third in range(3):
            dim = ORDERS[third][phase]
            h = rs_split(third)
            for sign in (0, 1):
                rs_push(third, sign, coord(dim, 2), h[sign], relay(third, sign, h[sign][1]))
        for third in range(3):
            dim = ORDERS[third][phase]
            h = rs_split(third)
            for sign in (0, 1):
                other = h[1 - sign]
                rs_push(third, 2 + sign, coord(dim, 1 if sign == 0 else -1), other,
                        stage(third, sign, other[0] - THIRDS[third][0], other[1]))
        for third in range(3):
            dim = ORDERS[third][phase]
            h = rs_split(third)
            for sign in (0, 1):
                q = coord(dim, 1 if sign == 0 else -1)
                landed(relay(third, sign, h[sign][1]), rs_recv.at[third, phase, sign])
                add_rows(phase, third, q, h[sign], [(ra[phase].at[third, sign], 0)])
                rs_push(third, 4 + sign, q, h[sign], stage(third, sign, h[sign][0] - THIRDS[third][0], h[sign][1]))
        for third in range(3):
            dim = ORDERS[third][phase]
            h = rs_split(third)
            for sign in (0, 1):
                other = h[1 - sign]
                landed(stage(third, sign, other[0] - THIRDS[third][0], other[1]), rs_recv.at[third, phase, 2 + sign])
                landed(stage(third, sign, h[sign][0] - THIRDS[third][0], h[sign][1]), rs_recv.at[third, phase, 4 + sign])
            add_rows(phase, third, me[dim], THIRDS[third], [(sa[phase].at[third, 0], 0), (sa[phase].at[third, 1], 0)])

    dkv_out[...] = dkv[me[0], me[1], me[2]].astype(BF)
    for copy in sends:
        copy.wait_send()


def attention(qt, q, dot_t, do, kv_loc, groups):
    lanes = 2 * groups * PIECE
    vmem = pl.BlockSpec(memory_space=pltpu.VMEM)
    return pl.pallas_call(
        functools.partial(kernel, groups),
        out_shape=(jax.ShapeDtypeStruct((HEAD_DIM, lanes), BF), jax.ShapeDtypeStruct((HEAD_DIM, lanes), BF),
                   jax.ShapeDtypeStruct((512, HEAD_DIM), BF)),
        in_specs=[vmem] * 5,
        out_specs=(vmem,) * 3,
        scratch_shapes=[
            pltpu.VMEM((4, 4, 4, 512, HEAD_DIM), BF),
            pltpu.VMEM((4, 4, 4, 512, HEAD_DIM), F32),
            pltpu.VMEM((1, lanes), F32), pltpu.VMEM((1, lanes), F32),
            pltpu.VMEM((HEAD_DIM, lanes), F32), pltpu.VMEM((HEAD_DIM, lanes), F32), pltpu.VMEM((1, lanes), F32),
            pltpu.VMEM((3, 2, 4, 4, 88, HEAD_DIM), F32), pltpu.VMEM((3, 2, 4, 88, HEAD_DIM), F32),
            pltpu.VMEM((3, 2, 88, HEAD_DIM), F32),
            pltpu.VMEM((3, 2, 4, 4, MAX_ROWS, HEAD_DIM), F32), pltpu.VMEM((3, 2, 4, MAX_ROWS, HEAD_DIM), F32),
            pltpu.VMEM((3, 2, MAX_ROWS, HEAD_DIM), F32),
            pltpu.SemaphoreType.DMA,
            pltpu.SemaphoreType.DMA((3, 3, 4)), pltpu.SemaphoreType.DMA((3, 3, 4)),
            pltpu.SemaphoreType.DMA((3, 3, 6)), pltpu.SemaphoreType.DMA((3, 3, 6)),
        ],
        compiler_params=pltpu.CompilerParams(collective_id=0, has_side_effects=True, vmem_limit_bytes=67043328),
        name='attention',
    )(qt, q, dot_t, do, kv_loc)


def dot_transposed(left, right):
    return lax.dot_general(left, right, (((1,), (1,)), ((), ())), preferred_element_type=F32)


def solution(mesh):
    row_spec = P(('dp', 'cp', 'tp'), None)

    def local_step(x_blk, dy_blk, w_query, w_key, w_value, w_out):
        groups = w_query.shape[1] // HEAD_DIM
        x_loc = lax.all_gather(x_blk, 'tp', axis=0, tiled=True)
        dy_loc = lax.all_gather(dy_blk, 'tp', axis=0, tiled=True)
        rows = x_loc.shape[0]

        def fold(a):
            return a.reshape(2, PIECE, groups, HEAD_DIM).transpose(0, 2, 1, 3).reshape(2 * groups * PIECE, HEAD_DIM)

        q = fold(jnp.dot(x_loc, w_query, preferred_element_type=F32).astype(BF))
        do = fold(dot_transposed(dy_loc, w_out).astype(BF))
        k = jnp.dot(x_loc, w_key, preferred_element_type=F32).astype(BF)
        v = jnp.dot(x_loc, w_value, preferred_element_type=F32).astype(BF)
        o_t, dq_t, dkv = attention(q.T, q, do.T, do, jnp.concatenate([k, v], axis=0), groups)

        def unfold(a):
            return a.reshape(HEAD_DIM, 2, groups, PIECE).transpose(1, 3, 2, 0).reshape(rows, groups * HEAD_DIM)

        y_part = jnp.dot(unfold(o_t), w_out, preferred_element_type=F32)
        y_blk = lax.psum_scatter(y_part, 'tp', scatter_dimension=0, tiled=True).astype(BF)
        dx_part = (dot_transposed(unfold(dq_t), w_query) + dot_transposed(dkv[:256], w_key)
                   + dot_transposed(dkv[256:], w_value))
        dx_blk = lax.psum_scatter(dx_part, 'tp', scatter_dimension=0, tiled=True).astype(BF)
        return y_blk, dx_blk

    return jax.shard_map(local_step, mesh=mesh,
                         in_specs=(row_spec, row_spec, P(None, 'tp'), P(None, 'tp'), P(None, 'tp'), P('tp', None)),
                         out_specs=(row_spec, row_spec), check_vma=False)
```

```python
import functools
import math

import jax
import jax.numpy as jnp
from jax import lax
from jax.experimental import pallas as pl
from jax.experimental.pallas import tpu as pltpu
from jax.sharding import PartitionSpec as P

HEAD_DIM = 128
PIECE = 128
SIDE = 4
LOG2E = math.log2(math.e)
LOWEST = float(jnp.finfo(jnp.float32).min)
MESH = pl.DeviceIdType.MESH
BF = jnp.bfloat16
F32 = jnp.float32
ALL = slice(None)

AG_ROWS = ((0, 160), (160, 176), (336, 176))
AG_HALF = (80, 96, 96)
RS_ROWS = ((0, 168), (168, 176), (344, 168))
RS_HALF = (88, 88, 88)
STRIDE = (16, 4, 1)
PLANES = (0, 1, 3, 2)
AG_RINGS = ('0a', '1a', '2a', '2b', '2c') + tuple(f'{t}{p}{o}' for t in (0, 1) for p in 'bc' for o in range(4))
RS_RINGS = {'0z': (0, 0, 0), '1z': (1, 0, 0), '2z': (2, 0, 2), '2x': (2, 2, 1), '2y': (2, 1, 0)}
for off in range(4):
    RS_RINGS[f'0x{off}'] = (0, 2, 1)
    RS_RINGS[f'1y{off}'] = (1, 1, 1)
    RS_RINGS[f'0y{off}'] = (0, 1, 0)
    RS_RINGS[f'1x{off}'] = (1, 2, 0)
RS_NAMES = tuple(RS_RINGS)


def dot(a, b):
    return lax.dot_general(a, b, (((1,), (0,)), ((), ())), preferred_element_type=F32)


def dot_ta(a, b):
    return lax.dot_general(a, b, (((0,), (0,)), ((), ())), preferred_element_type=F32)


def dot_tb(a, b):
    return lax.dot_general(a, b, (((1,), (1,)), ((), ())), preferred_element_type=F32)


def rs_scratch():
    shapes = []
    for part, _, free in RS_RINGS.values():
        lead = (SIDE,) * free
        shapes.append(pltpu.VMEM((2, *lead, RS_HALF[part], HEAD_DIM), F32))
        shapes.append(pltpu.VMEM((2, *lead, RS_ROWS[part][1], HEAD_DIM), F32))
    return shapes


def kernel(groups, *refs):
    (qt_ref, q_ref, dot_ref, do_ref, kv_loc, wq_hbm, wk_hbm, wv_hbm, wo_hbm, y_out, dx_out,
     kv, dkv, m_ref, l_ref, acc, delta, kt, vt, wq, wk, wv, wo, rows_bf, y_part, y_recv, dx_part, dx_recv,
     local_sem, pair_send, pair_recv, ag_send, ag_recv, rs_send, rs_recv, *rs_bufs) = refs
    rank = lax.axis_index('cp')
    core = lax.axis_index('tp')
    me = (rank // 16, lax.rem(rank // 4, 4), lax.rem(rank, 4))
    width = groups * PIECE
    dqt = acc

    coords = [[lax.rem(me[dim] + off, SIDE) for off in range(SIDE)] for dim in range(3)]

    def coord(dim, off):
        return coords[dim][off % SIDE]

    def device(dim, off):
        return {'cp': rank + STRIDE[dim] * (coord(dim, off) - me[dim])}

    partner = {'tp': 1 - core}
    barrier = pltpu.get_barrier_semaphore()
    for dim in range(3):
        for off in (1, -1):
            pl.semaphore_signal(barrier, inc=1, device_id=device(dim, off), device_id_type=MESH)
    pl.semaphore_signal(barrier, inc=1, device_id=partner, device_id_type=MESH)
    own = pltpu.make_async_copy(kv_loc, kv.at[me[0], me[1], me[2]], local_sem.at[0])
    own.start()
    loads = [pltpu.make_async_copy(src, dst, local_sem.at[1 + n])
             for n, (src, dst) in enumerate(((wq_hbm, wq), (wk_hbm, wk), (wv_hbm, wv), (wo_hbm, wo)))]
    for load in loads:
        load.start()
    pl.semaphore_wait(barrier, 7)
    own.wait()

    sends = []

    def remote(src, dst, send, recv, to):
        return pltpu.make_async_remote_copy(src_ref=src, dst_ref=dst, send_sem=send, recv_sem=recv,
                                            device_id=to, device_id_type=MESH)

    def push(src, dst, send, recv, to):
        remote(src, dst, send, recv, to).start()

    def landed(ref, sem):
        pltpu.make_async_copy(ref, ref, sem).wait()

    def ag_where(name):
        third = int(name[0])
        z, y, x = me
        if third == 2:
            if name[1] == 'a':
                return third, 1, lambda q: (z, q, x)
            if name[1] == 'b':
                return third, 2, lambda q: (z, ALL, q)
            return third, 0, lambda q: (q, ALL, ALL)
        if name[1] == 'a':
            return third, 0, lambda q: (q, y, x)
        plane = coord(0, int(name[2]))
        if third == 0:
            if name[1] == 'b':
                return third, 1, lambda q: (plane, q, x)
            return third, 2, lambda q: (plane, ALL, q)
        if name[1] == 'b':
            return third, 2, lambda q: (plane, y, q)
        return third, 1, lambda q: (plane, q, ALL)

    def ag_ref(name, off, rows):
        third, dim, where = ag_where(name)
        return kv.at[(*where(coord(dim, off)), pl.ds(*rows))]

    def ag_split(third):
        start, size = AG_ROWS[third]
        return (start, AG_HALF[third]), (start + AG_HALF[third], size - AG_HALF[third])

    def ag_push(name, kind, off, rows):
        n = AG_RINGS.index(name)
        ref = ag_ref(name, off, rows)
        push(ref, ref, ag_send.at[n, kind], ag_recv.at[n, kind], device(ag_where(name)[1], 1 if kind % 2 == 0 else -1))
        sends.append(lambda: (ag_ref(name, off, rows), ag_send.at[n, kind]))

    def direct(*names):
        for name in names:
            for kind in (0, 1):
                ag_push(name, kind, 0, AG_ROWS[int(name[0])])

    def relay(*names):
        for name in names:
            third = int(name[0])
            for kind in (0, 1):
                off = -1 if kind == 0 else 1
                landed(ag_ref(name, off, AG_ROWS[third]), ag_recv.at[AG_RINGS.index(name), kind])
                ag_push(name, 2 + kind, off, ag_split(third)[kind])

    def done(*names):
        for name in names:
            for kind in (0, 1):
                landed(ag_ref(name, 2, ag_split(int(name[0]))[kind]), ag_recv.at[AG_RINGS.index(name), 2 + kind])

    def rs_where(name):
        z, y, x = me
        part = int(name[0])
        if name in ('0z', '1z'):
            return lambda q: (q, y, x)
        if name == '2z':
            return lambda q: (q, ALL, ALL)
        if name == '2x':
            return lambda q: (z, ALL, q)
        if name == '2y':
            return lambda q: (z, q, x)
        plane = coord(0, int(name[2]))
        return {'0x': lambda q: (plane, ALL, q), '1y': lambda q: (plane, q, ALL),
                '0y': lambda q: (plane, q, x), '1x': lambda q: (plane, y, q)}[name[:2]]

    def rs_split(part):
        start, size = RS_ROWS[part]
        return (start, RS_HALF[part]), (start + RS_HALF[part], size - RS_HALF[part])

    def rs_ref(name, q, rows):
        return dkv.at[(*rs_where(name)(q), pl.ds(*rows))]

    def rs_land(name, kind, sign):
        part, _, free = RS_RINGS[name]
        n = RS_NAMES.index(name)
        h = rs_split(part)
        lead = (ALL,) * free
        if kind == 0:
            return rs_bufs[2 * n].at[(sign, *lead, pl.ds(0, h[sign][1]))]
        rows = h[1 - sign] if kind == 1 else h[sign]
        return rs_bufs[2 * n + 1].at[(sign, *lead, pl.ds(rows[0] - RS_ROWS[part][0], rows[1]))]

    def rs_push(name, kind, sign, q, rows):
        n = RS_NAMES.index(name)
        push(rs_ref(name, q, rows), rs_land(name, kind, sign), rs_send.at[n, 2 * kind + sign],
             rs_recv.at[n, 2 * kind + sign], device(RS_RINGS[name][1], 1 if sign == 0 else -1))
        off = 2 if kind == 0 else 1 if sign == 0 else -1
        sends.append(lambda: (rs_ref(name, coord(RS_RINGS[name][1], off), rows), rs_send.at[n, 2 * kind + sign]))

    def rs_landed(name, kind, sign):
        landed(rs_land(name, kind, sign), rs_recv.at[RS_NAMES.index(name), 2 * kind + sign])

    def rs_add(name, q, rows, sources):
        free = RS_RINGS[name][2]
        where = rs_where(name)(q)

        def one(u, carry):
            sub = [lax.rem(u // SIDE ** (free - 1 - n), SIDE) for n in range(free)]
            left = iter(sub)
            idx = tuple(next(left) if w is ALL else w for w in where)
            total = dkv[(*idx, slice(rows[0], rows[0] + rows[1]), ALL)]
            for ref, offset in sources:
                total = total + ref[(*sub, slice(offset, offset + rows[1]), ALL)]
            dkv[(*idx, slice(rows[0], rows[0] + rows[1]), ALL)] = total
            return carry

        if free:
            lax.fori_loop(0, SIDE ** free, one, 0)
        else:
            one(0, 0)

    def rs_far(name, signs=(0, 1)):
        part, dim, _ = RS_RINGS[name]
        for sign in signs:
            rs_push(name, 0, sign, coord(dim, 2), rs_split(part)[sign])

    def rs_raw(name, signs=(0, 1)):
        part, dim, _ = RS_RINGS[name]
        for sign in signs:
            rs_push(name, 1, sign, coord(dim, 1 if sign == 0 else -1), rs_split(part)[1 - sign])

    def rs_mid(name, signs=(0, 1)):
        part, dim, _ = RS_RINGS[name]
        n = RS_NAMES.index(name)
        for sign in signs:
            rows = rs_split(part)[sign]
            q = coord(dim, 1 if sign == 0 else -1)
            rs_landed(name, 0, sign)
            rs_add(name, q, rows, [(rs_bufs[2 * n].at[sign], 0)])
            rs_push(name, 2, sign, q, rows)

    def rs_fin(name):
        part, dim, _ = RS_RINGS[name]
        n = RS_NAMES.index(name)
        for kind in (1, 2):
            for sign in (0, 1):
                rs_landed(name, kind, sign)
        rs_add(name, me[dim], RS_ROWS[part], [(rs_bufs[2 * n + 1].at[0], 0), (rs_bufs[2 * n + 1].at[1], 0)])

    def each(f, *names):
        for name in names:
            f(name)

    def rs_start(name):
        rs_far(name)
        rs_raw(name)

    scale = HEAD_DIM ** -0.5
    c = scale * LOG2E

    def lanes_of(half):
        return pl.ds(pl.multiple_of(half * width, PIECE), width)

    def allowed(j0, second, half):
        row = lax.broadcasted_iota(jnp.int32, (512, 1), 0)
        b = row // PIECE
        kpiece = j0 + b + second * (127 - 2 * (j0 + b))
        kpos = kpiece * PIECE + lax.rem(row, PIECE)
        qpiece = rank + half * (127 - 2 * rank)
        qpos = qpiece * PIECE + lax.rem(lax.broadcasted_iota(jnp.int32, (1, width), 1), PIECE)
        return kpos <= qpos

    def fwd_tile(half, mask):
        ql = lanes_of(half)
        s = dot(kt[...], qt_ref[:, ql])
        if mask is not None:
            s = jnp.where(mask, s, LOWEST)
        m_old = m_ref[:, ql]
        m_new = jnp.maximum(m_old, jnp.max(s, axis=0, keepdims=True))
        alpha = jnp.exp2((m_old - m_new) * c)
        p = jnp.exp2((s - m_new) * c)
        if mask is not None:
            p = jnp.where(mask, p, 0.0)
        m_ref[:, ql] = m_new
        l_ref[:, ql] = l_ref[:, ql] * alpha + jnp.sum(p, axis=0, keepdims=True)
        acc[:, ql] = acc[:, ql] * alpha + dot_ta(vt[...], p.astype(BF))

    def bwd_tile(half, mask):
        ql = lanes_of(half)
        k = kt[...]
        p = jnp.exp2(dot(k, qt_ref[:, ql]) * c - m_ref[:, ql])
        if mask is not None:
            p = jnp.where(mask, p, 0.0)
        pb = p.astype(BF)
        ds = (pb.astype(F32) * (dot(vt[...], dot_ref[:, ql]) - delta[:, ql])).astype(BF)
        dqt[:, ql] += dot_ta(k, ds)
        return dot(ds, q_ref[ql, :]) * scale, dot(pb, do_ref[ql, :])

    def group_loop(zp, yp, body):
        here = zp * 4 + yp
        mine = me[0] * 4 + me[1]
        mixed = here == mine
        high = here > mine
        count = jnp.where(mixed, 3, 2)

        def step(u, carry):
            second = jnp.logical_and(mixed, u == 2)
            half = jnp.where(jnp.logical_or(high, u == 2), 1, u)
            masked = jnp.logical_and(mixed, u != 1)

            @pl.when(high)
            def _():
                kt[...] = kv[zp, yp, pl.ds(2 * u, 2), 0:256, :].reshape(512, HEAD_DIM)
                vt[...] = kv[zp, yp, pl.ds(2 * u, 2), 256:512, :].reshape(512, HEAD_DIM)

            @pl.when(jnp.logical_and(jnp.logical_not(high), jnp.logical_not(second)))
            def _():
                kt[...] = kv[zp, yp, :, 0:128, :].reshape(512, HEAD_DIM)
                vt[...] = kv[zp, yp, :, 256:384, :].reshape(512, HEAD_DIM)

            @pl.when(second)
            def _():
                kt[...] = kv[zp, yp, :, 128:256, :].reshape(512, HEAD_DIM)
                vt[...] = kv[zp, yp, :, 384:512, :].reshape(512, HEAD_DIM)

            body(u, here * 4, second, high, half, masked)
            return carry

        lax.fori_loop(0, count, step, 0)

    def fwd_group(zp, yp):
        def body(u, j0, second, high, half, masked):
            @pl.when(jnp.logical_not(masked))
            def _():
                fwd_tile(half, None)

            @pl.when(masked)
            def _():
                fwd_tile(half, allowed(j0, jnp.where(second, 1, 0), half))

        group_loop(zp, yp, body)

    def bwd_group(zp, yp):
        dkv[zp, yp] = jnp.zeros((SIDE, 512, HEAD_DIM), F32)

        def body(u, j0, second, high, half, masked):
            def keep(dk, dv):
                @pl.when(high)
                def _():
                    dkv[zp, yp, pl.ds(2 * u, 2), 0:256, :] = dk.reshape(2, 256, HEAD_DIM)
                    dkv[zp, yp, pl.ds(2 * u, 2), 256:512, :] = dv.reshape(2, 256, HEAD_DIM)

                @pl.when(jnp.logical_not(high))
                def _():
                    dkv[zp, yp, :, 0:128, :] += dk.reshape(4, 128, HEAD_DIM)
                    dkv[zp, yp, :, 256:384, :] += dv.reshape(4, 128, HEAD_DIM)

            @pl.when(jnp.logical_not(masked))
            def _():
                keep(*bwd_tile(half, None))

            @pl.when(masked)
            def _():
                dk, dv = bwd_tile(half, allowed(j0, jnp.where(second, 1, 0), half))

                @pl.when(second)
                def _():
                    dkv[zp, yp, :, 128:256, :] = dk.reshape(4, 128, HEAD_DIM)
                    dkv[zp, yp, :, 384:512, :] = dv.reshape(4, 128, HEAD_DIM)

                @pl.when(jnp.logical_not(second))
                def _():
                    dkv[zp, yp, :, 0:128, :] += dk.reshape(4, 128, HEAD_DIM)
                    dkv[zp, yp, :, 256:384, :] += dv.reshape(4, 128, HEAD_DIM)

        group_loop(zp, yp, body)

    def run(compute, reverse, events):
        def step(g, carry):
            for at, ops in events.items():
                @pl.when(g == at)
                def _():
                    for f, *names in ops:
                        f(*names)
            d = g // 4
            if reverse:
                d = 3 - d
            off = d + d // 2 - 2 * (d // 3)
            compute(lax.rem(me[0] + off, SIDE), lax.rem(g, 4))
            return carry

        lax.fori_loop(0, 16, step, 0)

    m_ref[...] = jnp.full(m_ref.shape, LOWEST, F32)
    l_ref[...] = jnp.zeros(l_ref.shape, F32)
    acc[...] = jnp.zeros(acc.shape, F32)
    direct('0b0', '1b0', '2a', '0a', '1a')
    relay('0b0', '1b0', '2a', '0a', '1a')
    done('0b0')
    direct('0c0')
    done('1b0')
    direct('1c0')
    done('2a')
    direct('2b')
    direct('0b1', '1b1', '0b3', '1b3')
    relay('0c0', '1c0', '2b')
    relay('0b1', '1b1', '0b3', '1b3')
    done('2b')
    direct('2c')
    done('0b1')
    direct('0c1')
    done('1b1')
    direct('1c1')
    done('0b3', '1b3')
    direct('0c3', '1c3')
    done('0c0', '1c0')
    run(fwd_group, False, {
        1: [(done, '0a', '1a'), (direct, '0b2', '1b2'), (relay, '0c1', '1c1')],
        2: [(relay, '0b2', '1b2'), (relay, '0c3', '1c3')],
        3: [(done, '0b2', '1b2'), (direct, '0c2', '1c2')],
        4: [(done, '0c1', '1c1'), (relay, '2c')],
        6: [(relay, '0c2', '1c2')],
        8: [(done, '0c3', '1c3')],
        12: [(done, '0c2', '1c2', '2c')],
    })

    l = l_ref[...]
    o = (acc[...] * (1.0 / l)).astype(BF)
    delta[...] = jnp.sum(dot_ref[...].astype(F32) * o.astype(F32), axis=0, keepdims=True)
    m_ref[...] = m_ref[...] * c + jnp.log(l) * LOG2E

    def to_rows(value_t):
        for s in range(2):
            for h in range(groups):
                lo = (s * groups + h) * PIECE
                rows_bf[s, :, h * HEAD_DIM:(h + 1) * HEAD_DIM] = value_t[:, lo:lo + PIECE].T

    for load in loads:
        load.wait()
    to_rows(o)
    y_part[0] = dot(rows_bf[1 - core], wo[...])
    y_copy = remote(y_part.at[0], y_recv, pair_send.at[0], pair_recv.at[0], partner)
    y_copy.start()
    y_part[1] = dot(rows_bf[core], wo[...])

    dqt[...] = jnp.zeros(dqt.shape, F32)
    both = (0, 1)
    run(bwd_group, True, {
        4: [(rs_far, '0x2'), (rs_far, '1y2'), (rs_far, '2z'), (rs_raw, '0x2'), (rs_raw, '1y2')],
        6: [(rs_mid, '0x2'), (rs_mid, '1y2')],
        8: [(rs_start, '0x3'), (rs_start, '1y3'), (rs_raw, '2z', (1,)), (rs_mid, '2z', (1,)),
            (rs_fin, '0x2'), (rs_start, '0y2'), (rs_fin, '1y2'), (rs_start, '1x2')],
        10: [(rs_mid, '0x3'), (rs_mid, '1y3'), (rs_mid, '0y2'), (rs_mid, '1x2')],
        12: [(rs_start, '0x1'), (rs_start, '1y1'), (rs_raw, '2z', (0,)), (rs_mid, '2z', (0,)),
             (rs_fin, '0y2'), (rs_fin, '1x2'), (rs_far, '0z'), (rs_far, '1z'),
             (rs_fin, '0x3'), (rs_start, '0y3'), (rs_fin, '1y3'), (rs_start, '1x3')],
        14: [(rs_mid, '0x1'), (rs_mid, '1y1'), (rs_mid, '0y3'), (rs_mid, '1x3')],
    })
    each(rs_start, '0x0', '1y0')
    rs_fin('0x1')
    rs_start('0y1')
    rs_fin('1y1')
    rs_start('1x1')
    each(rs_fin, '0y3', '1x3')
    for name in ('0z', '1z'):
        rs_raw(name, (1,))
        rs_mid(name, (1,))
    y_copy.wait_recv()
    y_out[...] = (y_part[1] + y_recv[...]).astype(BF)
    to_rows((dqt[...] * scale).astype(BF))
    dx_part[0] = dot_tb(rows_bf[1 - core], wq[...])
    each(rs_mid, '0x0', '1y0', '0y1', '1x1')
    rs_fin('2z')
    rs_start('2x')
    dx_part[1] = dot_tb(rows_bf[core], wq[...])
    each(rs_fin, '0y1', '1x1')
    for name in ('0z', '1z'):
        rs_raw(name, (0,))
        rs_mid(name, (0,))
    rs_fin('0x0')
    rs_start('0y0')
    rs_fin('1y0')
    rs_start('1x0')
    rs_mid('2x')
    each(rs_mid, '0y0', '1x0')
    rs_fin('2x')
    rs_start('2y')
    each(rs_fin, '0y0', '1x0')
    rs_mid('2y')
    each(rs_fin, '0z', '1z', '2y')

    dk_own = dkv[me[0], me[1], me[2], 0:256, :].astype(BF)
    dv_own = dkv[me[0], me[1], me[2], 256:512, :].astype(BF)
    kt[0:256, :] = dk_own
    vt[0:256, :] = dv_own

    def add_kv(slot, side):
        rows = pl.ds(pl.multiple_of(side * PIECE, PIECE), PIECE)
        dx_part[slot] = dx_part[slot] + dot_tb(kt[rows, :], wk[...]) + dot_tb(vt[rows, :], wv[...])

    add_kv(0, 1 - core)
    dx_copy = remote(dx_part.at[0], dx_recv, pair_send.at[1], pair_recv.at[1], partner)
    dx_copy.start()
    add_kv(1, core)
    for sent in sends:
        landed(*sent())
    y_copy.wait_send()
    dx_copy.wait_recv()
    dx_out[...] = (dx_part[1] + dx_recv[...]).astype(BF)
    dx_copy.wait_send()


def attention(qt, q, dot_t, do, kv_loc, w_query, w_key, w_value, w_out, groups):
    lanes = 2 * groups * PIECE
    dim = w_query.shape[0]
    vmem = pl.BlockSpec(memory_space=pltpu.VMEM)
    anywhere = pl.BlockSpec(memory_space=pl.ANY)
    weights = (w_query, w_key, w_value, w_out)
    return pl.pallas_call(
        functools.partial(kernel, groups),
        out_shape=(jax.ShapeDtypeStruct((PIECE, dim), BF),) * 2,
        in_specs=[vmem] * 5 + [anywhere] * 4,
        out_specs=(vmem,) * 2,
        scratch_shapes=[
            pltpu.VMEM((4, 4, 4, 512, HEAD_DIM), BF),
            pltpu.VMEM((4, 4, 4, 512, HEAD_DIM), F32),
            pltpu.VMEM((1, lanes), F32), pltpu.VMEM((1, lanes), F32),
            pltpu.VMEM((HEAD_DIM, lanes), F32), pltpu.VMEM((1, lanes), F32),
            pltpu.VMEM((512, HEAD_DIM), BF), pltpu.VMEM((512, HEAD_DIM), BF),
            *[pltpu.VMEM(w.shape, BF) for w in weights],
            pltpu.VMEM((2, PIECE, groups * HEAD_DIM), BF),
            pltpu.VMEM((2, PIECE, dim), F32), pltpu.VMEM((PIECE, dim), F32),
            pltpu.VMEM((2, PIECE, dim), F32), pltpu.VMEM((PIECE, dim), F32),
            pltpu.SemaphoreType.DMA((5,)),
            pltpu.SemaphoreType.DMA((2,)), pltpu.SemaphoreType.DMA((2,)),
            pltpu.SemaphoreType.DMA((len(AG_RINGS), 4)), pltpu.SemaphoreType.DMA((len(AG_RINGS), 4)),
            pltpu.SemaphoreType.DMA((len(RS_NAMES), 6)), pltpu.SemaphoreType.DMA((len(RS_NAMES), 6)),
            *rs_scratch(),
        ],
        compiler_params=pltpu.CompilerParams(collective_id=0, has_side_effects=True, vmem_limit_bytes=67043328),
        name='attention',
    )(qt, q, dot_t, do, kv_loc, *weights)


def solution(mesh):
    row_spec = P(('dp', 'cp', 'tp'), None)

    def local_step(x_blk, dy_blk, w_query, w_key, w_value, w_out):
        groups = w_query.shape[1] // HEAD_DIM
        x_loc = lax.all_gather(x_blk, 'tp', axis=0, tiled=True)
        dy_loc = lax.all_gather(dy_blk, 'tp', axis=0, tiled=True)

        def fold(a):
            return a.reshape(2, PIECE, groups, HEAD_DIM).transpose(0, 2, 1, 3).reshape(2 * groups * PIECE, HEAD_DIM)

        q = fold(jnp.dot(x_loc, w_query, preferred_element_type=F32).astype(BF))
        do = fold(dot_tb(dy_loc, w_out).astype(BF))
        k = jnp.dot(x_loc, w_key, preferred_element_type=F32).astype(BF)
        v = jnp.dot(x_loc, w_value, preferred_element_type=F32).astype(BF)
        return attention(q.T, q, do.T, do, jnp.concatenate([k, v], axis=0), w_query, w_key, w_value, w_out, groups)

    return jax.shard_map(local_step, mesh=mesh,
                         in_specs=(row_spec, row_spec, P(None, 'tp'), P(None, 'tp'), P(None, 'tp'), P('tp', None)),
                         out_specs=(row_spec, row_spec), check_vma=False)
```

```python
import collections
import functools
import math

import jax
import jax.numpy as jnp
from jax import lax
from jax.experimental import pallas as pl
from jax.experimental.pallas import tpu as pltpu
from jax.sharding import PartitionSpec as P

HEAD_DIM = 128
PIECE = 128
SIDE = 4
LOG2E = math.log2(math.e)
LOWEST = float(jnp.finfo(jnp.float32).min)
MESH = pl.DeviceIdType.MESH
BF = jnp.bfloat16
F32 = jnp.float32
ALL = slice(None)

AG_ROWS = ((0, 160), (160, 192), (352, 160))
AG_HALF = (80, 96, 80)
RS_ROWS = ((0, 160), (160, 160), (320, 192), (320, 96), (416, 96))
RS_HALF = (80, 80, 96, 48, 48)
STRIDE = (16, 4, 1)
AG_RINGS = ('0a', '1a', '2a', '1c0') + tuple(n + str(o) for n in ('0b', '1b', '0r', '2b', '2c') for o in range(4)) + tuple(
    n + str(o) for n in ('0c', '1c') for o in range(1, 4))
RS_RINGS = {'0z': (0, 0, 0), '1z': (1, 0, 0), '3x': (3, 2, 1), '3y': (3, 1, 0), '4y': (4, 1, 1), '4x': (4, 2, 0)}
for off in range(4):
    RS_RINGS[f'2z{off}'] = (2, 0, 1)
    RS_RINGS[f'1y{off}'] = (1, 1, 1)
    RS_RINGS[f'0y{off}'] = (0, 1, 0)
    RS_RINGS[f'1x{off}'] = (1, 2, 0)
    for row in range(4):
        RS_RINGS[f'0x{off}{row}'] = (0, 2, 0)
RS_NAMES = tuple(RS_RINGS)


def dot(a, b):
    return lax.dot_general(a, b, (((1,), (0,)), ((), ())), preferred_element_type=F32)


def dot_ta(a, b):
    return lax.dot_general(a, b, (((0,), (0,)), ((), ())), preferred_element_type=F32)


def dot_tb(a, b):
    return lax.dot_general(a, b, (((1,), (1,)), ((), ())), preferred_element_type=F32)


def rs_scratch():
    shapes = []
    for part, _, free in RS_RINGS.values():
        lead = (SIDE,) * free
        shapes.append(pltpu.VMEM((2, *lead, RS_HALF[part], HEAD_DIM), F32))
        shapes.append(pltpu.VMEM((2, *lead, RS_ROWS[part][1], HEAD_DIM), F32))
    return shapes


def kernel(groups, *refs):
    (x_hbm, dy_hbm, wq_hbm, wk_hbm, wv_hbm, wo_hbm, y_out, dx_out, xs, dys, qt_ref, q_ref, dot_ref, do_ref,
     kv, dkv, m_ref, l_ref, acc, delta, kt, vt, wq, wk, wv, wo, rows_bf, y_part, y_recv, dx_part, dx_recv,
     local_sem, pair_send, pair_recv, ag_send, ag_recv, rs_send, rs_recv, *rs_bufs) = refs
    rank = lax.axis_index('cp')
    core = lax.axis_index('tp')
    me = (rank // 16, lax.rem(rank // 4, 4), lax.rem(rank, 4))
    width = groups * PIECE
    dqt = acc

    coords = [[lax.rem(me[dim] + off, SIDE) for off in range(SIDE)] for dim in range(3)]

    def coord(dim, off):
        return coords[dim][off % SIDE]

    def device(dim, off):
        return {'cp': rank + STRIDE[dim] * (coord(dim, off) - me[dim])}

    partner = {'tp': 1 - core}
    barrier = pltpu.get_barrier_semaphore()
    for dim in range(3):
        for off in (1, -1):
            pl.semaphore_signal(barrier, inc=1, device_id=device(dim, off), device_id_type=MESH)
    pl.semaphore_signal(barrier, inc=1, device_id=partner, device_id_type=MESH)
    loads = {name: pltpu.make_async_copy(src, dst, local_sem.at[n]) for n, (name, src, dst) in enumerate((
        ('x', x_hbm, xs.at[core]), ('wk', wk_hbm, wk), ('wv', wv_hbm, wv), ('dy', dy_hbm, dys.at[core]),
        ('wq', wq_hbm, wq), ('wo', wo_hbm, wo)))}
    for load in loads.values():
        load.start()
    pl.semaphore_wait(barrier, 7)

    sends = []

    def remote(src, dst, send, recv, to):
        return pltpu.make_async_remote_copy(src_ref=src, dst_ref=dst, send_sem=send, recv_sem=recv,
                                            device_id=to, device_id_type=MESH)

    def push(src, dst, send, recv, to):
        remote(src, dst, send, recv, to).start()

    def landed(ref, sem):
        pltpu.make_async_copy(ref, ref, sem).wait()

    def ag_where(name):
        third = int(name[0])
        z, y, x = me
        if name[1] == 'a':
            return (third, 1, lambda q: (z, q, x)) if third == 2 else (third, 0, lambda q: (q, y, x))
        off = int(name[2])
        if name[1] == 'r' or name[:2] == '2b':
            row = coord(1, off)
            return third, 2, lambda q: (z, row, q)
        if third == 2:
            column = coord(2, off)
            return third, 0, lambda q: (q, ALL, column)
        plane = coord(0, off)
        if third == 0:
            if name[1] == 'b':
                return third, 1, lambda q: (plane, q, x)
            return third, 2, lambda q: (plane, ALL, q)
        if name[1] == 'b':
            return third, 2, lambda q: (plane, y, q)
        return third, 1, lambda q: (plane, q, ALL)

    def ag_ref(name, off, rows):
        third, dim, where = ag_where(name)
        return kv.at[(*where(coord(dim, off)), pl.ds(*rows))]

    def ag_split(third):
        start, size = AG_ROWS[third]
        return (start, AG_HALF[third]), (start + AG_HALF[third], size - AG_HALF[third])

    def ag_push(name, kind, off, rows):
        n = AG_RINGS.index(name)
        ref = ag_ref(name, off, rows)
        push(ref, ref, ag_send.at[n, kind], ag_recv.at[n, kind], device(ag_where(name)[1], 1 if kind % 2 == 0 else -1))
        sends.append(lambda: (ag_ref(name, off, rows), ag_send.at[n, kind]))

    def direct(*names):
        for name in names:
            for kind in (0, 1):
                ag_push(name, kind, 0, AG_ROWS[int(name[0])])

    def relay(*names):
        for name in names:
            third = int(name[0])
            for kind in (0, 1):
                off = -1 if kind == 0 else 1
                landed(ag_ref(name, off, AG_ROWS[third]), ag_recv.at[AG_RINGS.index(name), kind])
                ag_push(name, 2 + kind, off, ag_split(third)[kind])

    def done(*names):
        for name in names:
            for kind in (0, 1):
                landed(ag_ref(name, 2, ag_split(int(name[0]))[kind]), ag_recv.at[AG_RINGS.index(name), 2 + kind])

    def rs_where(name):
        z, y, x = me
        if name in ('0z', '1z'):
            return lambda q: (q, y, x)
        if name == '3x':
            return lambda q: (z, ALL, q)
        if name == '3y':
            return lambda q: (z, q, x)
        if name == '4y':
            return lambda q: (z, q, ALL)
        if name == '4x':
            return lambda q: (z, y, q)
        if name[:2] == '2z':
            row = coord(1, int(name[2]))
            return lambda q: (q, row, ALL)
        plane = coord(0, int(name[2]))
        if name[:2] == '0x':
            row = coord(1, int(name[3]))
            return lambda q: (plane, row, q)
        return {'1y': lambda q: (plane, q, ALL), '0y': lambda q: (plane, q, x), '1x': lambda q: (plane, y, q)}[name[:2]]

    def rs_split(part):
        start, size = RS_ROWS[part]
        return (start, RS_HALF[part]), (start + RS_HALF[part], size - RS_HALF[part])

    def rs_ref(name, q, rows):
        return dkv.at[(*rs_where(name)(q), pl.ds(*rows))]

    def rs_land(name, kind, sign):
        part, _, free = RS_RINGS[name]
        n = RS_NAMES.index(name)
        h = rs_split(part)
        lead = (ALL,) * free
        if kind == 0:
            return rs_bufs[2 * n].at[(sign, *lead, pl.ds(0, h[sign][1]))]
        rows = h[1 - sign] if kind == 1 else h[sign]
        return rs_bufs[2 * n + 1].at[(sign, *lead, pl.ds(rows[0] - RS_ROWS[part][0], rows[1]))]

    def rs_push(name, kind, sign, q, rows):
        n = RS_NAMES.index(name)
        push(rs_ref(name, q, rows), rs_land(name, kind, sign), rs_send.at[n, 2 * kind + sign],
             rs_recv.at[n, 2 * kind + sign], device(RS_RINGS[name][1], 1 if sign == 0 else -1))
        off = 2 if kind == 0 else 1 if sign == 0 else -1
        sends.append(lambda: (rs_ref(name, coord(RS_RINGS[name][1], off), rows), rs_send.at[n, 2 * kind + sign]))

    def rs_landed(name, kind, sign):
        landed(rs_land(name, kind, sign), rs_recv.at[RS_NAMES.index(name), 2 * kind + sign])

    def rs_add(name, q, rows, sources):
        free = RS_RINGS[name][2]
        where = rs_where(name)(q)

        def one(u, carry):
            sub = [lax.rem(u // SIDE ** (free - 1 - n), SIDE) for n in range(free)]
            left = iter(sub)
            idx = tuple(next(left) if w is ALL else w for w in where)
            total = dkv[(*idx, slice(rows[0], rows[0] + rows[1]), ALL)]
            for ref, offset in sources:
                total = total + ref[(*sub, slice(offset, offset + rows[1]), ALL)]
            dkv[(*idx, slice(rows[0], rows[0] + rows[1]), ALL)] = total
            return carry

        if free:
            lax.fori_loop(0, SIDE ** free, one, 0)
        else:
            one(0, 0)

    def rs_far(name, signs=(0, 1)):
        part, dim, _ = RS_RINGS[name]
        for sign in signs:
            rs_push(name, 0, sign, coord(dim, 2), rs_split(part)[sign])

    def rs_raw(name, signs=(0, 1)):
        part, dim, _ = RS_RINGS[name]
        for sign in signs:
            rs_push(name, 1, sign, coord(dim, 1 if sign == 0 else -1), rs_split(part)[1 - sign])

    def rs_mid(name, signs=(0, 1)):
        part, dim, _ = RS_RINGS[name]
        n = RS_NAMES.index(name)
        for sign in signs:
            rows = rs_split(part)[sign]
            q = coord(dim, 1 if sign == 0 else -1)
            rs_landed(name, 0, sign)
            rs_add(name, q, rows, [(rs_bufs[2 * n].at[sign], 0)])
            rs_push(name, 2, sign, q, rows)

    def rs_fin(name):
        part, dim, _ = RS_RINGS[name]
        n = RS_NAMES.index(name)
        for kind in (1, 2):
            for sign in (0, 1):
                rs_landed(name, kind, sign)
        rs_add(name, me[dim], RS_ROWS[part], [(rs_bufs[2 * n + 1].at[0], 0), (rs_bufs[2 * n + 1].at[1], 0)])

    def each(f, *names):
        for name in names:
            f(name)

    def rs_start(name):
        rs_far(name)
        rs_raw(name)

    scale = HEAD_DIM ** -0.5
    c = scale * LOG2E

    def lanes_of(half):
        return pl.ds(pl.multiple_of(half * width, PIECE), width)

    def allowed(j0, second, half):
        row = lax.broadcasted_iota(jnp.int32, (512, 1), 0)
        b = row // PIECE
        kpiece = j0 + b + second * (127 - 2 * (j0 + b))
        kpos = kpiece * PIECE + lax.rem(row, PIECE)
        qpiece = rank + half * (127 - 2 * rank)
        qpos = qpiece * PIECE + lax.rem(lax.broadcasted_iota(jnp.int32, (1, width), 1), PIECE)
        return kpos <= qpos

    def scores(k, ql, mask=None):
        s = dot(k, qt_ref[:, ql])
        return s if mask is None else jnp.where(mask, s, LOWEST)

    def online(s, v, ql, mask=None):
        m_old = m_ref[:, ql]
        m_new = jnp.maximum(m_old, jnp.max(s, axis=0, keepdims=True))
        alpha = jnp.exp2((m_old - m_new) * c)
        p = jnp.exp2((s - m_new) * c)
        if mask is not None:
            p = jnp.where(mask, p, 0.0)
        m_ref[:, ql] = m_new
        l_ref[:, ql] = l_ref[:, ql] * alpha + jnp.sum(p, axis=0, keepdims=True)
        acc[:, ql] = acc[:, ql] * alpha + dot_ta(v, p.astype(BF))

    def bwd_tile(half, mask):
        ql = lanes_of(half)
        k = kt[...]
        p = jnp.exp2(dot(k, qt_ref[:, ql]) * c - m_ref[:, ql])
        if mask is not None:
            p = jnp.where(mask, p, 0.0)
        pb = p.astype(BF)
        ds = (pb.astype(F32) * (dot(vt[...], dot_ref[:, ql]) - delta[:, ql])).astype(BF)
        dqt[:, ql] += dot_ta(k, ds)
        return dot(ds, q_ref[ql, :]) * scale, dot(pb, do_ref[ql, :])

    def group_loop(zp, yp, body):
        here = zp * 4 + yp
        mine = me[0] * 4 + me[1]
        mixed = here == mine
        high = here > mine
        count = jnp.where(mixed, 3, 2)

        def step(u, carry):
            second = jnp.logical_and(mixed, u == 2)
            half = jnp.where(jnp.logical_or(high, u == 2), 1, u)
            masked = jnp.logical_and(mixed, u != 1)

            @pl.when(high)
            def _():
                kt[...] = kv[zp, yp, pl.ds(2 * u, 2), 0:256, :].reshape(512, HEAD_DIM)
                vt[...] = kv[zp, yp, pl.ds(2 * u, 2), 256:512, :].reshape(512, HEAD_DIM)

            @pl.when(jnp.logical_and(jnp.logical_not(high), jnp.logical_not(second)))
            def _():
                kt[...] = kv[zp, yp, :, 0:128, :].reshape(512, HEAD_DIM)
                vt[...] = kv[zp, yp, :, 256:384, :].reshape(512, HEAD_DIM)

            @pl.when(second)
            def _():
                kt[...] = kv[zp, yp, :, 128:256, :].reshape(512, HEAD_DIM)
                vt[...] = kv[zp, yp, :, 384:512, :].reshape(512, HEAD_DIM)

            body(u, here * 4, second, high, half, masked)
            return carry

        lax.fori_loop(0, count, step, 0)

    def fwd_group(zp, yp):
        here = zp * 4 + yp
        mine = me[0] * 4 + me[1]
        first, last = slice(0, width), slice(width, 2 * width)

        @pl.when(here < mine)
        def _():
            k = kv[zp, yp, :, 0:128, :].reshape(512, HEAD_DIM)
            v = kv[zp, yp, :, 256:384, :].reshape(512, HEAD_DIM)
            s0, s1 = scores(k, first), scores(k, last)
            online(s0, v, first)
            online(s1, v, last)

        @pl.when(here > mine)
        def _():
            pairs = (slice(0, 2), slice(2, 4))
            s0, s1 = (scores(kv[zp, yp, pair, 0:256, :].reshape(512, HEAD_DIM), last) for pair in pairs)
            for s, pair in zip((s0, s1), pairs):
                online(s, kv[zp, yp, pair, 256:512, :].reshape(512, HEAD_DIM), last)

        def body(u, j0, second, high, half, masked):
            ql = lanes_of(half)
            mask = allowed(j0, jnp.where(second, 1, 0), half)
            online(scores(kt[...], ql, mask), vt[...], ql, mask)

        @pl.when(here == mine)
        def _():
            group_loop(zp, yp, body)

    def bwd_group(zp, yp):
        def first(dk, dv):
            none = jnp.zeros((SIDE, 128, HEAD_DIM), F32)
            dkv[zp, yp, :, 0:128, :] = dk.reshape(4, 128, HEAD_DIM)
            dkv[zp, yp, :, 128:256, :] = none
            dkv[zp, yp, :, 256:384, :] = dv.reshape(4, 128, HEAD_DIM)
            dkv[zp, yp, :, 384:512, :] = none

        def body(u, j0, second, high, half, masked):
            def keep(dk, dv):
                @pl.when(high)
                def _():
                    dkv[zp, yp, pl.ds(2 * u, 2), 0:256, :] = dk.reshape(2, 256, HEAD_DIM)
                    dkv[zp, yp, pl.ds(2 * u, 2), 256:512, :] = dv.reshape(2, 256, HEAD_DIM)

                @pl.when(jnp.logical_and(jnp.logical_not(high), u == 0))
                def _():
                    first(dk, dv)

                @pl.when(jnp.logical_and(jnp.logical_not(high), u != 0))
                def _():
                    dkv[zp, yp, :, 0:128, :] += dk.reshape(4, 128, HEAD_DIM)
                    dkv[zp, yp, :, 256:384, :] += dv.reshape(4, 128, HEAD_DIM)

            @pl.when(jnp.logical_not(masked))
            def _():
                keep(*bwd_tile(half, None))

            @pl.when(masked)
            def _():
                dk, dv = bwd_tile(half, allowed(j0, jnp.where(second, 1, 0), half))

                @pl.when(second)
                def _():
                    dkv[zp, yp, :, 128:256, :] = dk.reshape(4, 128, HEAD_DIM)
                    dkv[zp, yp, :, 384:512, :] = dv.reshape(4, 128, HEAD_DIM)

                @pl.when(jnp.logical_not(second))
                def _():
                    first(dk, dv)

        group_loop(zp, yp, body)

    def spiral(n):
        return n + n // 2 - 2 * (n // 3)

    def run(compute, reverse, events):
        def step(g, carry):
            for at, ops in events.items():
                @pl.when(g == at)
                def _():
                    for f, *args in ops:
                        f(*args)
            d, r = g // 4, lax.rem(g, 4)
            if reverse:
                d, r = 3 - d, 3 - r
            compute(lax.rem(me[0] + spiral(d), SIDE), lax.rem(me[1] + spiral(r), SIDE))
            return carry

        lax.fori_loop(0, 16, step, 0)

    m_ref[...] = jnp.full(m_ref.shape, LOWEST, F32)
    l_ref[...] = jnp.zeros(l_ref.shape, F32)
    acc[...] = jnp.zeros(acc.shape, F32)
    loads['x'].wait()
    x_copy = remote(xs.at[core], xs.at[core], pair_send.at[2], pair_recv.at[2], partner)
    x_copy.start()
    loads['wk'].wait()
    loads['wv'].wait()

    def project_kv(slot):
        rows = xs[slot]
        lo = pl.multiple_of(slot * PIECE, PIECE)
        kv[me[0], me[1], me[2], pl.ds(lo, PIECE), :] = dot(rows, wk[...]).astype(BF)
        kv[me[0], me[1], me[2], pl.ds(256 + lo, PIECE), :] = dot(rows, wv[...]).astype(BF)

    def spread(rows, slot, flat, flat_t):
        for h in range(groups):
            block = rows[:, h * HEAD_DIM:(h + 1) * HEAD_DIM]
            lo = pl.multiple_of((slot * groups + h) * PIECE, PIECE)
            flat[pl.ds(lo, PIECE), :] = block
            flat_t[:, pl.ds(lo, PIECE)] = block.T

    def project_q(slot):
        spread(dot(xs[slot], wq[...]).astype(BF), slot, q_ref, qt_ref)

    def project_do(slot):
        spread(dot_tb(dys[slot], wo[...]).astype(BF), slot, do_ref, dot_ref)

    project_kv(core)
    landed(xs.at[1 - core], pair_recv.at[2])
    project_kv(1 - core)
    direct('0r0', '1b0', '2b0', '0b0', '2a', '0a', '1a')
    loads['dy'].wait()
    dy_copy = remote(dys.at[core], dys.at[core], pair_send.at[3], pair_recv.at[3], partner)
    dy_copy.start()
    loads['wq'].wait()
    project_q(core)
    relay('1b0', '0r0', '0b0', '2a', '2b0')
    direct('0r1', '0r3', '2b1', '2b3')
    project_q(1 - core)
    done('1b0')
    direct('1c0')
    relay('0a', '1a')
    direct('0b1', '1b1', '0b3', '1b3')
    done('0b0')
    direct('0r2')
    done('2a')
    direct('2b2', '2c0')
    done('0r0', '2b0')
    run(fwd_group, False, {
        1: [(relay, '0r1', '2b1', '0r3', '2b3', '1c0'), (loads['wo'].wait,), (project_do, core),
            (relay, '0b1', '1b1', '0b3', '1b3'), (done, '0r1', '2b1')],
        2: [(relay, '0r2', '2b2'), (direct, '2c1', '2c3'), (done, '0b1'), (direct, '0c1'), (done, '1b1'), (direct, '1c1'),
            (done, '0b3'), (direct, '0c3'), (done, '1b3'), (direct, '1c3'), (done, '0r3', '2b3')],
        3: [(relay, '2c0'), (done, '0a', '1a'), (direct, '0b2', '1b2'), (done, '0r2', '2b2', '1c0'), (direct, '2c2'),
            (landed, dys.at[1 - core], pair_recv.at[3]), (project_do, 1 - core), (relay, '0c1', '1c1')],
        4: [(relay, '2c1', '2c3', '2c2'), (done, '0c1', '1c1')],
        5: [(relay, '0c3', '1c3'), (relay, '0b2', '1b2')],
        7: [(done, '0b2', '1b2'), (direct, '0c2', '1c2')],
        8: [(done, '0c3', '1c3')],
        10: [(relay, '0c2', '1c2')],
        12: [(done, '0c2', '1c2', '2c0', '2c1', '2c2', '2c3')],
    })
    x_copy.wait_send()
    dy_copy.wait_send()

    l = l_ref[...]
    o = (acc[...] * (1.0 / l)).astype(BF)
    delta[...] = jnp.sum(dot_ref[...].astype(F32) * o.astype(F32), axis=0, keepdims=True)
    m_ref[...] = m_ref[...] * c + jnp.log(l) * LOG2E

    def to_rows(value_t):
        for s in range(2):
            for h in range(groups):
                lo = (s * groups + h) * PIECE
                rows_bf[s, :, h * HEAD_DIM:(h + 1) * HEAD_DIM] = value_t[:, lo:lo + PIECE].T

    to_rows(o)
    y_part[0] = dot(rows_bf[1 - core], wo[...])
    y_copy = remote(y_part.at[0], y_recv, pair_send.at[0], pair_recv.at[0], partner)
    y_copy.start()
    y_part[1] = dot(rows_bf[core], wo[...])

    dqt[...] = jnp.zeros(dqt.shape, F32)
    plan = collections.defaultdict(list)

    def at(time, rank_in_time, f, *args):
        plan[time].append((rank_in_time, len(plan[time]), (f, *args)))

    for p, o in enumerate((2, 3, 1, 0)):
        for k, r in enumerate((2, 3, 1, 0)):
            t = 4 * p + k + 1
            sign = (1,) if k == 1 else (0,)
            side = (1,) if p == 1 else (0,)
            row = f'0x{o}{r}'
            at(t, 0, rs_start, row)
            at(t + 2, 1, rs_mid, row)
            at(t + 4, 2, rs_fin, row)
            if p == 0:
                at(t, 0, rs_far, f'2z{r}')
            elif p < 3:
                at(t, 0, rs_raw, f'2z{r}', side)
                at(t, 1, rs_mid, f'2z{r}', side)
            else:
                at(18, 2, rs_fin, f'2z{r}')
            if k == 0:
                at(t, 0, rs_far, f'1y{o}')
                at(t + 4, 3, rs_far, f'0y{o}')
            elif k < 3:
                at(t, 0, rs_raw, f'1y{o}', sign)
                at(t + 1, 1, rs_mid, f'1y{o}', sign)
                at(t + 4, 3, rs_raw, f'0y{o}', sign)
                at(t + 5, 1, rs_mid, f'0y{o}', sign)
            else:
                at(t + 3, 2, rs_fin, f'1y{o}')
                at(t + 3, 3, rs_start, f'1x{o}')
                at(t + 5, 1, rs_mid, f'1x{o}')
                for late, name, last in ((6, '0z', f'0y{o}'), (7, '1z', f'1x{o}')):
                    at(t + late, 2, rs_fin, last)
                    if p == 0:
                        at(t + late, 3, rs_far, name)
                    elif p < 3:
                        at(t + late, 3, rs_raw, name, side)
                        at(21, 1, rs_mid, name, side)
                    else:
                        at(24, 2, rs_fin, name)
    for name in ('3x', '4y'):
        at(18, 3, rs_start, name)
        at(20, 1, rs_mid, name)
        at(21, 2, rs_fin, name)
    for name in ('3y', '4x'):
        at(21, 3, rs_start, name)
        at(22, 1, rs_mid, name)
        at(24, 2, rs_fin, name)
    plan = {time: [op for _, _, op in sorted(ops, key=lambda e: e[:2])] for time, ops in sorted(plan.items())}
    run(bwd_group, True, {time: ops for time, ops in plan.items() if time < 16})

    def dx_start():
        y_copy.wait_recv()
        y_out[...] = (y_part[1] + y_recv[...]).astype(BF)
        to_rows((dqt[...] * scale).astype(BF))
        dx_part[0] = dot_tb(rows_bf[1 - core], wq[...])

    for time, ops in plan.items():
        if time >= 16:
            for f, *args in ops:
                f(*args)
            if time == 16:
                dx_start()
            if time == 17:
                dx_part[1] = dot_tb(rows_bf[core], wq[...])

    dk_own = dkv[me[0], me[1], me[2], 0:256, :].astype(BF)
    dv_own = dkv[me[0], me[1], me[2], 256:512, :].astype(BF)
    kt[0:256, :] = dk_own
    vt[0:256, :] = dv_own

    def add_kv(slot, side):
        rows = pl.ds(pl.multiple_of(side * PIECE, PIECE), PIECE)
        dx_part[slot] = dx_part[slot] + dot_tb(kt[rows, :], wk[...]) + dot_tb(vt[rows, :], wv[...])

    add_kv(0, 1 - core)
    dx_copy = remote(dx_part.at[0], dx_recv, pair_send.at[1], pair_recv.at[1], partner)
    dx_copy.start()
    add_kv(1, core)
    for sent in sends:
        landed(*sent())
    y_copy.wait_send()
    dx_copy.wait_recv()
    dx_out[...] = (dx_part[1] + dx_recv[...]).astype(BF)
    dx_copy.wait_send()


def attention(x_blk, dy_blk, w_query, w_key, w_value, w_out, groups):
    lanes = 2 * groups * PIECE
    dim = w_query.shape[0]
    vmem = pl.BlockSpec(memory_space=pltpu.VMEM)
    anywhere = pl.BlockSpec(memory_space=pl.ANY)
    weights = (w_query, w_key, w_value, w_out)
    return pl.pallas_call(
        functools.partial(kernel, groups),
        out_shape=(jax.ShapeDtypeStruct((PIECE, dim), BF),) * 2,
        in_specs=[anywhere] * 6,
        out_specs=(vmem,) * 2,
        scratch_shapes=[
            pltpu.VMEM((2, *x_blk.shape), BF), pltpu.VMEM((2, *x_blk.shape), BF),
            *[pltpu.VMEM(shape, BF) for shape in ((HEAD_DIM, lanes), (lanes, HEAD_DIM)) * 2],
            pltpu.VMEM((4, 4, 4, 512, HEAD_DIM), BF),
            pltpu.VMEM((4, 4, 4, 512, HEAD_DIM), F32),
            pltpu.VMEM((1, lanes), F32), pltpu.VMEM((1, lanes), F32),
            pltpu.VMEM((HEAD_DIM, lanes), F32), pltpu.VMEM((1, lanes), F32),
            pltpu.VMEM((512, HEAD_DIM), BF), pltpu.VMEM((512, HEAD_DIM), BF),
            *[pltpu.VMEM(w.shape, BF) for w in weights],
            pltpu.VMEM((2, PIECE, groups * HEAD_DIM), BF),
            pltpu.VMEM((2, PIECE, dim), F32), pltpu.VMEM((PIECE, dim), F32),
            pltpu.VMEM((2, PIECE, dim), F32), pltpu.VMEM((PIECE, dim), F32),
            pltpu.SemaphoreType.DMA((6,)),
            pltpu.SemaphoreType.DMA((4,)), pltpu.SemaphoreType.DMA((4,)),
            pltpu.SemaphoreType.DMA((len(AG_RINGS), 4)), pltpu.SemaphoreType.DMA((len(AG_RINGS), 4)),
            pltpu.SemaphoreType.DMA((len(RS_NAMES), 6)), pltpu.SemaphoreType.DMA((len(RS_NAMES), 6)),
            *rs_scratch(),
        ],
        compiler_params=pltpu.CompilerParams(collective_id=0, has_side_effects=True, vmem_limit_bytes=67043328),
        name='attention',
    )(x_blk, dy_blk, *weights)


def solution(mesh):
    row_spec = P(('dp', 'cp', 'tp'), None)

    def local_step(x_blk, dy_blk, w_query, w_key, w_value, w_out):
        groups = w_query.shape[1] // HEAD_DIM
        return attention(x_blk, dy_blk, w_query, w_key, w_value, w_out, groups)

    return jax.shard_map(local_step, mesh=mesh,
                         in_specs=(row_spec, row_spec, P(None, 'tp'), P(None, 'tp'), P(None, 'tp'), P('tp', None)),
                         out_specs=(row_spec, row_spec), check_vma=False)
```

```python
import collections
import functools
import math

import jax
import jax.numpy as jnp
from jax import lax
from jax.experimental import pallas as pl
from jax.experimental.pallas import tpu as pltpu
from jax.sharding import PartitionSpec as P

HEAD_DIM = 128
PIECE = 128
SIDE = 4
LOG2E = math.log2(math.e)
LOWEST = float(jnp.finfo(jnp.float32).min)
MESH = pl.DeviceIdType.MESH
BF = jnp.bfloat16
F32 = jnp.float32
ALL = slice(None)

BOTH = (0, 1)
TORUS = (SIDE,) * 3
BLOCK = 4 * PIECE
KEY_A, KEY_B, VAL_A, VAL_B = (slice(n * PIECE, (n + 1) * PIECE) for n in range(SIDE))
KEYS, VALUES = slice(0, 2 * PIECE), slice(2 * PIECE, BLOCK)
SPIRAL = (0, 1, 3, 2)
INWARD = (2, 3, 1, 0)

AG_ROWS = ((0, 160), (160, 192), (352, 160))
AG_HALF = (80, 96, 80)
RS_ROWS = ((0, 160), (160, 160), (320, 192), (320, 96), (416, 96))
RS_HALF = (80, 80, 96, 48, 48)
STRIDE = (16, 4, 1)
AG_RINGS = ('0a', '1a', '2a') + tuple(n + str(o) for n in ('0b', '1b', '0r', '2b', '2c', '0c', '1c') for o in range(SIDE))
RS_RINGS = {'0z': (0, 0, 0), '1z': (1, 0, 0), '3y': (3, 1, 0), '4y': (4, 1, 1), '4x': (4, 2, 0)}
for off in range(SIDE):
    RS_RINGS[f'2z{off}'] = (2, 0, 1)
    RS_RINGS[f'1y{off}'] = (1, 1, 1)
    RS_RINGS[f'0y{off}'] = (0, 1, 0)
    RS_RINGS[f'1x{off}'] = (1, 2, 0)
    RS_RINGS[f'3x{off}'] = (3, 2, 0)
    for row in range(SIDE):
        RS_RINGS[f'0x{off}{row}'] = (0, 2, 0)
RS_NAMES = tuple(RS_RINGS)


def dot(a, b):
    return lax.dot_general(a, b, (((1,), (0,)), ((), ())), preferred_element_type=F32)


def dot_ta(a, b):
    return lax.dot_general(a, b, (((0,), (0,)), ((), ())), preferred_element_type=F32)


def dot_tb(a, b):
    return lax.dot_general(a, b, (((1,), (1,)), ((), ())), preferred_element_type=F32)


def rs_scratch():
    shapes = []
    for part, _, free in RS_RINGS.values():
        lead = (SIDE,) * free
        shapes.append(pltpu.VMEM((2, *lead, RS_HALF[part], HEAD_DIM), F32))
        shapes.append(pltpu.VMEM((2, *lead, RS_ROWS[part][1], HEAD_DIM), F32))
    return shapes


def kernel(groups, *refs):
    (x_hbm, dy_hbm, wq_hbm, wk_hbm, wv_hbm, wo_hbm, y_out, dx_out, xs, dys, qt_ref, q_ref, dot_ref, do_ref,
     kv, dkv, m_ref, l_ref, acc, delta, kt, vt, wq, wk, wv, wo, rows_bf, y_part, y_recv, dx_part, dx_recv,
     local_sem, pair_send, pair_recv, ag_send, ag_recv, rs_send, rs_recv, *rs_bufs) = refs
    rank = lax.axis_index('cp')
    core = lax.axis_index('tp')
    me = mz, my, mx = (rank // STRIDE[0], lax.rem(rank // SIDE, SIDE), lax.rem(rank, SIDE))
    width = groups * PIECE
    dqt = acc

    coords = [[lax.rem(me[dim] + off, SIDE) for off in range(SIDE)] for dim in range(3)]

    def coord(dim, off):
        return coords[dim][off % SIDE]

    def device(dim, off):
        return {'cp': rank + STRIDE[dim] * (coord(dim, off) - me[dim])}

    partner = {'tp': 1 - core}
    barrier = pltpu.get_barrier_semaphore()
    for dim in range(3):
        for off in (1, -1):
            pl.semaphore_signal(barrier, inc=1, device_id=device(dim, off), device_id_type=MESH)
    pl.semaphore_signal(barrier, inc=1, device_id=partner, device_id_type=MESH)
    loads = {name: pltpu.make_async_copy(src, dst, local_sem.at[n]) for n, (name, src, dst) in enumerate((
        ('x', x_hbm, xs.at[core]), ('wk', wk_hbm, wk), ('wv', wv_hbm, wv), ('dy', dy_hbm, dys.at[core]),
        ('wq', wq_hbm, wq), ('wo', wo_hbm, wo)))}
    for load in loads.values():
        load.start()
    pl.semaphore_wait(barrier, 7)

    sends = []

    def remote(src, dst, send, recv, to):
        return pltpu.make_async_remote_copy(src_ref=src, dst_ref=dst, send_sem=send, recv_sem=recv,
                                            device_id=to, device_id_type=MESH)

    def push(src, dst, send, recv, to):
        remote(src, dst, send, recv, to).start()

    def landed(ref, sem):
        pltpu.make_async_copy(ref, ref, sem).wait()

    def ag_where(name):
        third = int(name[0])
        if name[1] == 'a':
            return (third, 1, lambda q: (mz, q, mx)) if third == 2 else (third, 0, lambda q: (q, my, mx))
        off = int(name[2])
        if name[1] == 'r' or name[:2] == '2b':
            row = coord(1, off)
            return third, 2, lambda q: (mz, row, q)
        if third == 2:
            column = coord(2, off)
            return third, 0, lambda q: (q, ALL, column)
        plane = coord(0, off)
        if third == 0:
            if name[1] == 'b':
                return third, 1, lambda q: (plane, q, mx)
            return third, 2, lambda q: (plane, ALL, q)
        if name[1] == 'b':
            return third, 2, lambda q: (plane, my, q)
        return third, 1, lambda q: (plane, q, ALL)

    def ag_ref(name, off, rows):
        third, dim, where = ag_where(name)
        return kv.at[(*where(coord(dim, off)), pl.ds(*rows))]

    def ag_split(third):
        start, size = AG_ROWS[third]
        return (start, AG_HALF[third]), (start + AG_HALF[third], size - AG_HALF[third])

    def ag_push(name, kind, off, rows):
        n = AG_RINGS.index(name)
        ref = ag_ref(name, off, rows)
        push(ref, ref, ag_send.at[n, kind], ag_recv.at[n, kind], device(ag_where(name)[1], 1 if kind % 2 == 0 else -1))
        sends.append(lambda: (ag_ref(name, off, rows), ag_send.at[n, kind]))

    def direct(*names):
        for name in names:
            for kind in BOTH:
                ag_push(name, kind, 0, AG_ROWS[int(name[0])])

    def relay(*names):
        for name in names:
            third = int(name[0])
            for kind in BOTH:
                off = -1 if kind == 0 else 1
                landed(ag_ref(name, off, AG_ROWS[third]), ag_recv.at[AG_RINGS.index(name), kind])
                ag_push(name, 2 + kind, off, ag_split(third)[kind])

    def done(*names):
        for name in names:
            for kind in BOTH:
                landed(ag_ref(name, 2, ag_split(int(name[0]))[kind]), ag_recv.at[AG_RINGS.index(name), 2 + kind])

    def rs_where(name):
        if name in ('0z', '1z'):
            return lambda q: (q, my, mx)
        if name[:2] == '3x':
            row = coord(1, int(name[2]))
            return lambda q: (mz, row, q)
        if name == '3y':
            return lambda q: (mz, q, mx)
        if name == '4y':
            return lambda q: (mz, q, ALL)
        if name == '4x':
            return lambda q: (mz, my, q)
        if name[:2] == '2z':
            row = coord(1, int(name[2]))
            return lambda q: (q, row, ALL)
        plane = coord(0, int(name[2]))
        if name[:2] == '0x':
            row = coord(1, int(name[3]))
            return lambda q: (plane, row, q)
        return {'1y': lambda q: (plane, q, ALL), '0y': lambda q: (plane, q, mx), '1x': lambda q: (plane, my, q)}[name[:2]]

    def rs_split(part):
        start, size = RS_ROWS[part]
        return (start, RS_HALF[part]), (start + RS_HALF[part], size - RS_HALF[part])

    def rs_ref(name, q, rows):
        return dkv.at[(*rs_where(name)(q), pl.ds(*rows))]

    def rs_land(name, kind, sign):
        part, _, free = RS_RINGS[name]
        n = RS_NAMES.index(name)
        h = rs_split(part)
        lead = (ALL,) * free
        if kind == 0:
            return rs_bufs[2 * n].at[(sign, *lead, pl.ds(0, h[sign][1]))]
        rows = h[1 - sign] if kind == 1 else h[sign]
        return rs_bufs[2 * n + 1].at[(sign, *lead, pl.ds(rows[0] - RS_ROWS[part][0], rows[1]))]

    def rs_push(name, kind, sign, q, rows):
        n = RS_NAMES.index(name)
        push(rs_ref(name, q, rows), rs_land(name, kind, sign), rs_send.at[n, 2 * kind + sign],
             rs_recv.at[n, 2 * kind + sign], device(RS_RINGS[name][1], 1 if sign == 0 else -1))
        off = 2 if kind == 0 else 1 if sign == 0 else -1
        sends.append(lambda: (rs_ref(name, coord(RS_RINGS[name][1], off), rows), rs_send.at[n, 2 * kind + sign]))

    def rs_landed(name, kind, sign):
        landed(rs_land(name, kind, sign), rs_recv.at[RS_NAMES.index(name), 2 * kind + sign])

    def rs_add(name, q, rows, sources):
        free = RS_RINGS[name][2]
        where = rs_where(name)(q)

        def one(u, carry):
            sub = [lax.rem(u // SIDE ** (free - 1 - n), SIDE) for n in range(free)]
            left = iter(sub)
            idx = tuple(next(left) if w is ALL else w for w in where)
            total = dkv[(*idx, slice(rows[0], rows[0] + rows[1]), ALL)]
            for ref, offset in sources:
                total = total + ref[(*sub, slice(offset, offset + rows[1]), ALL)]
            dkv[(*idx, slice(rows[0], rows[0] + rows[1]), ALL)] = total
            return carry

        if free:
            lax.fori_loop(0, SIDE ** free, one, 0)
        else:
            one(0, 0)

    def rs_far(name, signs=BOTH):
        part, dim, _ = RS_RINGS[name]
        for sign in signs:
            rs_push(name, 0, sign, coord(dim, 2), rs_split(part)[sign])

    def rs_raw(name, signs=BOTH):
        part, dim, _ = RS_RINGS[name]
        for sign in signs:
            rs_push(name, 1, sign, coord(dim, 1 if sign == 0 else -1), rs_split(part)[1 - sign])

    def rs_mid(name, signs=BOTH):
        part, dim, _ = RS_RINGS[name]
        n = RS_NAMES.index(name)
        for sign in signs:
            rows = rs_split(part)[sign]
            q = coord(dim, 1 if sign == 0 else -1)
            rs_landed(name, 0, sign)
            rs_add(name, q, rows, [(rs_bufs[2 * n].at[sign], 0)])
            rs_push(name, 2, sign, q, rows)

    def rs_fin(name):
        part, dim, _ = RS_RINGS[name]
        n = RS_NAMES.index(name)
        for kind in (1, 2):
            for sign in BOTH:
                rs_landed(name, kind, sign)
        rs_add(name, me[dim], RS_ROWS[part], [(rs_bufs[2 * n + 1].at[0], 0), (rs_bufs[2 * n + 1].at[1], 0)])

    def each(f, *names):
        for name in names:
            f(name)

    def rs_start(name):
        rs_far(name)
        rs_raw(name)

    scale = HEAD_DIM ** -0.5
    c = scale * LOG2E

    def lanes_of(half):
        return pl.ds(pl.multiple_of(half * width, PIECE), width)

    def allowed(j0, second, half):
        row = lax.broadcasted_iota(jnp.int32, (512, 1), 0)
        b = row // PIECE
        kpiece = j0 + b + second * (127 - 2 * (j0 + b))
        kpos = kpiece * PIECE + lax.rem(row, PIECE)
        qpiece = rank + half * (127 - 2 * rank)
        qpos = qpiece * PIECE + lax.rem(lax.broadcasted_iota(jnp.int32, (1, width), 1), PIECE)
        return kpos <= qpos

    def scores(k, ql, mask=None):
        s = dot(k, qt_ref[:, ql])
        return s if mask is None else jnp.where(mask, s, LOWEST)

    def online(s, v, ql, mask=None):
        m_old = m_ref[:, ql]
        m_new = jnp.maximum(m_old, jnp.max(s, axis=0, keepdims=True))
        alpha = jnp.exp2((m_old - m_new) * c)
        p = jnp.exp2((s - m_new) * c)
        if mask is not None:
            p = jnp.where(mask, p, 0.0)
        m_ref[:, ql] = m_new
        l_ref[:, ql] = l_ref[:, ql] * alpha + jnp.sum(p, axis=0, keepdims=True)
        acc[:, ql] = acc[:, ql] * alpha + dot_ta(v, p.astype(BF))

    def bwd_tile(half, mask):
        ql = lanes_of(half)
        k = kt[...]
        p = jnp.exp2(dot(k, qt_ref[:, ql]) * c - m_ref[:, ql])
        if mask is not None:
            p = jnp.where(mask, p, 0.0)
        pb = p.astype(BF)
        ds = (pb.astype(F32) * (dot(vt[...], dot_ref[:, ql]) - delta[:, ql])).astype(BF)
        dqt[:, ql] += dot_ta(k, ds)
        return dot(ds, q_ref[ql, :]) * scale, dot(pb, do_ref[ql, :])

    def group_loop(zp, yp, body):
        here = zp * SIDE + yp
        mine = mz * SIDE + my
        mixed = here == mine
        high = here > mine
        count = jnp.where(mixed, 3, 2)

        def step(u, carry):
            second = jnp.logical_and(mixed, u == 2)
            half = jnp.where(jnp.logical_or(high, u == 2), 1, u)
            masked = jnp.logical_and(mixed, u != 1)

            @pl.when(high)
            def _():
                kt[...] = kv[zp, yp, pl.ds(2 * u, 2), KEYS, :].reshape(BLOCK, HEAD_DIM)
                vt[...] = kv[zp, yp, pl.ds(2 * u, 2), VALUES, :].reshape(BLOCK, HEAD_DIM)

            @pl.when(jnp.logical_and(jnp.logical_not(high), jnp.logical_not(second)))
            def _():
                kt[...] = kv[zp, yp, :, KEY_A, :].reshape(BLOCK, HEAD_DIM)
                vt[...] = kv[zp, yp, :, VAL_A, :].reshape(BLOCK, HEAD_DIM)

            @pl.when(second)
            def _():
                kt[...] = kv[zp, yp, :, KEY_B, :].reshape(BLOCK, HEAD_DIM)
                vt[...] = kv[zp, yp, :, VAL_B, :].reshape(BLOCK, HEAD_DIM)

            body(u, here * 4, second, high, half, masked)
            return carry

        lax.fori_loop(0, count, step, 0)

    def fwd_group(zp, yp):
        here = zp * SIDE + yp
        mine = mz * SIDE + my
        first, last = slice(0, width), slice(width, 2 * width)

        @pl.when(here < mine)
        def _():
            k = kv[zp, yp, :, KEY_A, :].reshape(BLOCK, HEAD_DIM)
            v = kv[zp, yp, :, VAL_A, :].reshape(BLOCK, HEAD_DIM)
            s0, s1 = scores(k, first), scores(k, last)
            online(s0, v, first)
            online(s1, v, last)

        @pl.when(here > mine)
        def _():
            pairs = (slice(0, 2), slice(2, 4))
            s0, s1 = (scores(kv[zp, yp, pair, KEYS, :].reshape(BLOCK, HEAD_DIM), last) for pair in pairs)
            for s, pair in zip((s0, s1), pairs):
                online(s, kv[zp, yp, pair, VALUES, :].reshape(BLOCK, HEAD_DIM), last)

        def body(u, j0, second, high, half, masked):
            ql = lanes_of(half)
            mask = allowed(j0, jnp.where(second, 1, 0), half)
            online(scores(kt[...], ql, mask), vt[...], ql, mask)

        @pl.when(here == mine)
        def _():
            group_loop(zp, yp, body)

    def bwd_group(zp, yp):
        def first(dk, dv):
            none = jnp.zeros((SIDE, PIECE, HEAD_DIM), F32)
            dkv[zp, yp, :, KEY_A, :] = dk.reshape(SIDE, PIECE, HEAD_DIM)
            dkv[zp, yp, :, KEY_B, :] = none
            dkv[zp, yp, :, VAL_A, :] = dv.reshape(SIDE, PIECE, HEAD_DIM)
            dkv[zp, yp, :, VAL_B, :] = none

        def body(u, j0, second, high, half, masked):
            def keep(dk, dv):
                @pl.when(high)
                def _():
                    dkv[zp, yp, pl.ds(2 * u, 2), KEYS, :] = dk.reshape(2, 2 * PIECE, HEAD_DIM)
                    dkv[zp, yp, pl.ds(2 * u, 2), VALUES, :] = dv.reshape(2, 2 * PIECE, HEAD_DIM)

                @pl.when(jnp.logical_and(jnp.logical_not(high), u == 0))
                def _():
                    first(dk, dv)

                @pl.when(jnp.logical_and(jnp.logical_not(high), u != 0))
                def _():
                    dkv[zp, yp, :, KEY_A, :] += dk.reshape(SIDE, PIECE, HEAD_DIM)
                    dkv[zp, yp, :, VAL_A, :] += dv.reshape(SIDE, PIECE, HEAD_DIM)

            @pl.when(jnp.logical_not(masked))
            def _():
                keep(*bwd_tile(half, None))

            @pl.when(masked)
            def _():
                dk, dv = bwd_tile(half, allowed(j0, jnp.where(second, 1, 0), half))

                @pl.when(second)
                def _():
                    dkv[zp, yp, :, KEY_B, :] = dk.reshape(SIDE, PIECE, HEAD_DIM)
                    dkv[zp, yp, :, VAL_B, :] = dv.reshape(SIDE, PIECE, HEAD_DIM)

                @pl.when(jnp.logical_not(second))
                def _():
                    first(dk, dv)

        group_loop(zp, yp, body)

    def spiral(n):
        return n + n // 2 - 2 * (n // 3)

    def run(compute, reverse, events):
        def step(g, carry):
            for at, ops in events.items():
                @pl.when(g == at)
                def _():
                    for f, *args in ops:
                        f(*args)
            d, r = g // 4, lax.rem(g, 4)
            if reverse:
                d, r = 3 - d, 3 - r
            compute(lax.rem(mz + spiral(d), SIDE), lax.rem(my + spiral(r), SIDE))
            return carry

        lax.fori_loop(0, 16, step, 0)

    m_ref[...] = jnp.full(m_ref.shape, LOWEST, F32)
    l_ref[...] = jnp.zeros(l_ref.shape, F32)
    acc[...] = jnp.zeros(acc.shape, F32)
    loads['x'].wait()
    x_copy = remote(xs.at[core], xs.at[core], pair_send.at[2], pair_recv.at[2], partner)
    x_copy.start()
    loads['wk'].wait()
    loads['wv'].wait()

    def project_kv(slot):
        rows = xs[slot]
        lo = pl.multiple_of(slot * PIECE, PIECE)
        kv[*me, pl.ds(lo, PIECE), :] = dot(rows, wk[...]).astype(BF)
        kv[*me, pl.ds(256 + lo, PIECE), :] = dot(rows, wv[...]).astype(BF)

    def spread(rows, slot, flat, flat_t):
        for h in range(groups):
            block = rows[:, h * HEAD_DIM:(h + 1) * HEAD_DIM]
            lo = pl.multiple_of((slot * groups + h) * PIECE, PIECE)
            flat[pl.ds(lo, PIECE), :] = block
            flat_t[:, pl.ds(lo, PIECE)] = block.T

    def project_q(slot):
        spread(dot(xs[slot], wq[...]).astype(BF), slot, q_ref, qt_ref)

    def project_do(slot):
        spread(dot_tb(dys[slot], wo[...]).astype(BF), slot, do_ref, dot_ref)

    project_kv(core)
    landed(xs.at[1 - core], pair_recv.at[2])
    project_kv(1 - core)
    direct('0r0', '1b0', '2b0', '0b0', '2a', '0a', '1a')
    loads['dy'].wait()
    dy_copy = remote(dys.at[core], dys.at[core], pair_send.at[3], pair_recv.at[3], partner)
    dy_copy.start()
    loads['wq'].wait()
    project_q(core)
    relay('1b0', '0r0', '0b0', '2a', '2b0')
    direct('0r1', '0r3', '2b1', '2b3')
    project_q(1 - core)
    relay('0a', '1a')
    direct('0b1', '1b1', '0b3', '1b3')
    done('1b0')
    direct('1c0')
    done('0b0')
    direct('0r2')
    done('2a')
    direct('2b2', '2c0')
    done('0r0', '2b0')
    run(fwd_group, False, {
        1: [(relay, '0b1', '1b1', '0b3', '1b3'), (done, '0a', '1a'), (direct, '0b2', '1b2'),
            (relay, '0r1', '2b1', '0r3', '2b3', '2b2'), (direct, '2c1', '2c3'), (relay, '1c0'),
            (done, '0b1'), (direct, '0c1'), (done, '1b1'), (direct, '1c1'),
            (loads['wo'].wait,), (project_do, core), (done, '0r1', '2b1')],
        2: [(relay, '0r2'), (done, '2b3', '2b2'), (direct, '2c2'),
            (done, '0b3'), (direct, '0c3'), (done, '1b3'), (direct, '1c3'), (relay, '0b2', '1b2'), (done, '0r3')],
        3: [(relay, '2c0'), (done, '0r2', '1c0'),
            (landed, dys.at[1 - core], pair_recv.at[3]), (project_do, 1 - core), (relay, '0c1', '1c1'),
            (done, '0b2', '1b2'), (direct, '0c2', '1c2')],
        4: [(relay, '2c1', '2c3', '2c2'), (done, '0c1', '1c1')],
        5: [(relay, '0c3', '1c3')],
        7: [(relay, '0c2', '1c2')],
        8: [(done, '0c3', '1c3')],
        12: [(done, '0c2', '1c2', '2c0', '2c1', '2c2', '2c3')],
    })
    x_copy.wait_send()
    dy_copy.wait_send()

    l = l_ref[...]
    o = (acc[...] * (1.0 / l)).astype(BF)
    delta[...] = jnp.sum(dot_ref[...].astype(F32) * o.astype(F32), axis=0, keepdims=True)
    m_ref[...] = m_ref[...] * c + jnp.log(l) * LOG2E

    def to_rows(value_t):
        for s in range(2):
            for h in range(groups):
                lo = (s * groups + h) * PIECE
                rows_bf[s, :, h * HEAD_DIM:(h + 1) * HEAD_DIM] = value_t[:, lo:lo + PIECE].T

    to_rows(o)
    y_copy = remote(y_part.at[0], y_recv, pair_send.at[0], pair_recv.at[0], partner)

    dqt[...] = jnp.zeros(dqt.shape, F32)
    plan = collections.defaultdict(list)

    def at(time, rank_in_time, f, *args):
        plan[time].append((rank_in_time, len(plan[time]), (f, *args)))

    low, up = (1,), (0,)
    for p, o in enumerate(INWARD):
        for k, r in enumerate(INWARD):
            t = SIDE * p + k + 1
            sign = low if k == 1 else up
            side = low if p == 1 else up
            row = f'0x{o}{r}'
            at(t, 0, rs_start, row)
            at(t + 2, 1, rs_mid, row)
            at(t + 4, 2, rs_fin, row)
            if p == 0:
                at(t, 0, rs_far, f'2z{r}')
            elif p < 3:
                at(t, 0, rs_raw, f'2z{r}', side)
                at(t, 1, rs_mid, f'2z{r}', side)
            if k == 0:
                at(t, 0, rs_far, f'1y{o}')
                at(t + 4, 3, rs_far, f'0y{o}')
            elif k < 3:
                at(t, 0, rs_raw, f'1y{o}', sign)
                at(t + 1, 1, rs_mid, f'1y{o}', sign)
                at(t + 4, 3, rs_raw, f'0y{o}', sign)
                at(t + 5, 1, rs_mid, f'0y{o}', sign)
            else:
                at(t + 3, 2, rs_fin, f'1y{o}')
                at(t + 3, 3, rs_start, f'1x{o}')
                at(t + 5, 1, rs_mid, f'1x{o}')
                for late, name, last in ((6, '0z', f'0y{o}'), (7, '1z', f'1x{o}')):
                    at(t + late, 2, rs_fin, last)
                    if p == 0:
                        at(t + late, 3, rs_far, name)
                    elif p < 3:
                        at(t + late, 3, rs_raw, name, side)
                        at(21, 1, rs_mid, name, side)
                    else:
                        at(24, 2, rs_fin, name)
    for t, r, f, more in ((15, 2, rs_far, None), (17, 3, rs_raw, low), (18, 1, rs_raw, up), (19, 0, None, None)):
        at(t, 4, rs_fin, f'2z{r}')
        at(t, 5, rs_start, f'3x{r}')
        at(t + 2, 1, rs_mid, f'3x{r}')
        at(t + 3, 2, rs_fin, f'3x{r}')
        if f is None:
            at(20, 2, rs_fin, '4y')
            at(20, 2, rs_start, '4x')
            at(21, 1, rs_mid, '4x')
        else:
            for start, name, rank_in_time in ((t, '4y', 5), (t + 3, '3y', 2)):
                if more is None:
                    at(start, rank_in_time, f, name)
                else:
                    at(start, rank_in_time, f, name, more)
                    at(start + 1, 0, rs_mid, name, more)
    for name in ('3y', '4x'):
        at(23, 2, rs_fin, name)
    plan = {time: [op for _, _, op in sorted(ops, key=lambda e: e[:2])] for time, ops in sorted(plan.items())}
    run(bwd_group, True, {time: ops for time, ops in plan.items() if time < 16})

    def dx_start():
        y_part[0] = dot(rows_bf[1 - core], wo[...])
        y_copy.start()
        y_part[1] = dot(rows_bf[core], wo[...])
        to_rows((dqt[...] * scale).astype(BF))
        dx_part[0] = dot_tb(rows_bf[1 - core], wq[...])

    for time, ops in plan.items():
        if time >= 16:
            for f, *args in ops:
                f(*args)
            if time == 16:
                dx_start()
            if time == 17:
                dx_part[1] = dot_tb(rows_bf[core], wq[...])
                y_copy.wait_recv()
                y_out[...] = (y_part[1] + y_recv[...]).astype(BF)

    dk_own = dkv[*me, KEYS, :].astype(BF)
    dv_own = dkv[*me, VALUES, :].astype(BF)
    kt[0:256, :] = dk_own
    vt[0:256, :] = dv_own

    def add_kv(slot, side):
        rows = pl.ds(pl.multiple_of(side * PIECE, PIECE), PIECE)
        dx_part[slot] = dx_part[slot] + dot_tb(kt[rows, :], wk[...]) + dot_tb(vt[rows, :], wv[...])

    add_kv(0, 1 - core)
    dx_copy = remote(dx_part.at[0], dx_recv, pair_send.at[1], pair_recv.at[1], partner)
    dx_copy.start()
    add_kv(1, core)
    for sent in sends:
        landed(*sent())
    y_copy.wait_send()
    dx_copy.wait_recv()
    dx_out[...] = (dx_part[1] + dx_recv[...]).astype(BF)
    dx_copy.wait_send()


def attention(x_blk, dy_blk, w_query, w_key, w_value, w_out, groups):
    lanes = 2 * groups * PIECE
    dim = w_query.shape[0]
    vmem = pl.BlockSpec(memory_space=pltpu.VMEM)
    anywhere = pl.BlockSpec(memory_space=pl.ANY)
    weights = (w_query, w_key, w_value, w_out)
    return pl.pallas_call(
        functools.partial(kernel, groups),
        out_shape=(jax.ShapeDtypeStruct((PIECE, dim), BF),) * 2,
        in_specs=[anywhere] * 6,
        out_specs=(vmem,) * 2,
        scratch_shapes=[
            pltpu.VMEM((2, *x_blk.shape), BF), pltpu.VMEM((2, *x_blk.shape), BF),
            *[pltpu.VMEM(shape, BF) for shape in ((HEAD_DIM, lanes), (lanes, HEAD_DIM)) * 2],
            pltpu.VMEM((*TORUS, BLOCK, HEAD_DIM), BF),
            pltpu.VMEM((*TORUS, BLOCK, HEAD_DIM), F32),
            pltpu.VMEM((1, lanes), F32), pltpu.VMEM((1, lanes), F32),
            pltpu.VMEM((HEAD_DIM, lanes), F32), pltpu.VMEM((1, lanes), F32),
            pltpu.VMEM((BLOCK, HEAD_DIM), BF), pltpu.VMEM((BLOCK, HEAD_DIM), BF),
            *[pltpu.VMEM(w.shape, BF) for w in weights],
            pltpu.VMEM((2, PIECE, groups * HEAD_DIM), BF),
            pltpu.VMEM((2, PIECE, dim), F32), pltpu.VMEM((PIECE, dim), F32),
            pltpu.VMEM((2, PIECE, dim), F32), pltpu.VMEM((PIECE, dim), F32),
            pltpu.SemaphoreType.DMA((6,)),
            pltpu.SemaphoreType.DMA((4,)), pltpu.SemaphoreType.DMA((4,)),
            pltpu.SemaphoreType.DMA((len(AG_RINGS), 4)), pltpu.SemaphoreType.DMA((len(AG_RINGS), 4)),
            pltpu.SemaphoreType.DMA((len(RS_NAMES), 6)), pltpu.SemaphoreType.DMA((len(RS_NAMES), 6)),
            *rs_scratch(),
        ],
        compiler_params=pltpu.CompilerParams(collective_id=0, has_side_effects=True, vmem_limit_bytes=67043328),
        name='attention',
    )(x_blk, dy_blk, *weights)


def handover(y, dx):
    def body(y_in, dx_in, y_end, dx_end):
        y_end[...] = y_in[...]
        dx_end[...] = dx_in[...]

    vmem = pl.BlockSpec(memory_space=pltpu.VMEM)
    shape = jax.ShapeDtypeStruct(y.shape, y.dtype)
    return pl.pallas_call(body, out_shape=(shape, shape), in_specs=[vmem] * 2, out_specs=(vmem,) * 2, name='handover')(y, dx)


def solution(mesh):
    row_spec = P(('dp', 'cp', 'tp'), None)

    def local_step(x_blk, dy_blk, w_query, w_key, w_value, w_out):
        groups = w_query.shape[1] // HEAD_DIM
        return handover(*attention(x_blk, dy_blk, w_query, w_key, w_value, w_out, groups))

    return jax.shard_map(local_step, mesh=mesh,
                         in_specs=(row_spec, row_spec, P(None, 'tp'), P(None, 'tp'), P(None, 'tp'), P('tp', None)),
                         out_specs=(row_spec, row_spec), check_vma=False)
```

```python
import collections
import functools
import math

import jax
import jax.numpy as jnp
from jax import lax
from jax.experimental import pallas as pl
from jax.experimental.pallas import tpu as pltpu
from jax.sharding import PartitionSpec as P

HEAD_DIM = 128
PIECE = 128
SIDE = 4
LOG2E = math.log2(math.e)
LOWEST = float(jnp.finfo(jnp.float32).min)
MESH = pl.DeviceIdType.MESH
BF = jnp.bfloat16
F32 = jnp.float32
ALL = slice(None)

BOTH = (0, 1)
TORUS = (SIDE,) * 3
BLOCK = 4 * PIECE
KEY_A, KEY_B, VAL_A, VAL_B = (slice(n * PIECE, (n + 1) * PIECE) for n in range(SIDE))
KEYS, VALUES = slice(0, 2 * PIECE), slice(2 * PIECE, BLOCK)
SPIRAL = (0, 1, 3, 2)
INWARD = (2, 3, 1, 0)

AG_ROWS = ((0, 160), (160, 192), (352, 160))
AG_HALF = (80, 96, 80)
RS_ROWS = ((0, 160), (160, 160), (320, 192), (320, 96), (416, 96))
RS_HALF = (80, 80, 96, 48, 48)
STRIDE = (16, 4, 1)
AG_RINGS = ('0a', '1a', '2a') + tuple(n + str(o) for n in ('0b', '1b', '0r', '2b', '2c', '0c', '1c') for o in range(SIDE))
RS_RINGS = {'0z': (0, 0, 0), '1z': (1, 0, 0), '3y': (3, 1, 0), '4y': (4, 1, 1), '4x': (4, 2, 0)}
for off in range(SIDE):
    RS_RINGS[f'2z{off}'] = (2, 0, 1)
    RS_RINGS[f'1y{off}'] = (1, 1, 1)
    RS_RINGS[f'0y{off}'] = (0, 1, 0)
    RS_RINGS[f'1x{off}'] = (1, 2, 0)
    RS_RINGS[f'3x{off}'] = (3, 2, 0)
    for row in range(SIDE):
        RS_RINGS[f'0x{off}{row}'] = (0, 2, 0)
RS_NAMES = tuple(RS_RINGS)


def dot(a, b):
    return lax.dot_general(a, b, (((1,), (0,)), ((), ())), preferred_element_type=F32)


def dot_ta(a, b):
    return lax.dot_general(a, b, (((0,), (0,)), ((), ())), preferred_element_type=F32)


def dot_tb(a, b):
    return lax.dot_general(a, b, (((1,), (1,)), ((), ())), preferred_element_type=F32)


def rs_scratch():
    shapes = []
    for part, _, free in RS_RINGS.values():
        lead = (SIDE,) * free
        shapes.append(pltpu.VMEM((2, *lead, RS_HALF[part], HEAD_DIM), F32))
        shapes.append(pltpu.VMEM((2, *lead, RS_ROWS[part][1], HEAD_DIM), F32))
    return shapes


def kernel(groups, *refs):
    (x_hbm, dy_hbm, wq_hbm, wk_hbm, wv_hbm, wo_hbm, y_out, dx_out, xs, dys, qt_ref, q_ref, dot_ref, do_ref,
     kv, dkv, m_ref, l_ref, acc, delta, kt, vt, wq, wk, wv, wo, rows_bf, y_part, y_recv, dx_part, dx_recv,
     local_sem, pair_send, pair_recv, ag_send, ag_recv, rs_send, rs_recv, *rs_bufs) = refs
    rank = lax.axis_index('cp')
    core = lax.axis_index('tp')
    me = mz, my, mx = (rank // STRIDE[0], lax.rem(rank // SIDE, SIDE), lax.rem(rank, SIDE))
    width = groups * PIECE
    dqt = acc

    coords = [[lax.rem(me[dim] + off, SIDE) for off in range(SIDE)] for dim in range(3)]

    def coord(dim, off):
        return coords[dim][off % SIDE]

    def device(dim, off):
        return {'cp': rank + STRIDE[dim] * (coord(dim, off) - me[dim])}

    partner = {'tp': 1 - core}
    barrier = pltpu.get_barrier_semaphore()
    for dim in range(3):
        for off in (1, -1):
            pl.semaphore_signal(barrier, inc=1, device_id=device(dim, off), device_id_type=MESH)
    pl.semaphore_signal(barrier, inc=1, device_id=partner, device_id_type=MESH)
    loads = {name: pltpu.make_async_copy(src, dst, local_sem.at[n]) for n, (name, src, dst) in enumerate((
        ('x', x_hbm, xs.at[core]), ('wk', wk_hbm, wk), ('wv', wv_hbm, wv), ('dy', dy_hbm, dys.at[core]),
        ('wq', wq_hbm, wq), ('wo', wo_hbm, wo)))}
    for load in loads.values():
        load.start()
    pl.semaphore_wait(barrier, 7)

    sends = []

    def remote(src, dst, send, recv, to):
        return pltpu.make_async_remote_copy(src_ref=src, dst_ref=dst, send_sem=send, recv_sem=recv,
                                            device_id=to, device_id_type=MESH)

    def push(src, dst, send, recv, to):
        remote(src, dst, send, recv, to).start()

    def landed(ref, sem):
        pltpu.make_async_copy(ref, ref, sem).wait()

    def ag_where(name):
        third = int(name[0])
        if name[1] == 'a':
            return (third, 1, lambda q: (mz, q, mx)) if third == 2 else (third, 0, lambda q: (q, my, mx))
        off = int(name[2])
        if name[1] == 'r' or name[:2] == '2b':
            row = coord(1, off)
            return third, 2, lambda q: (mz, row, q)
        if third == 2:
            column = coord(2, off)
            return third, 0, lambda q: (q, ALL, column)
        plane = coord(0, off)
        if third == 0:
            if name[1] == 'b':
                return third, 1, lambda q: (plane, q, mx)
            return third, 2, lambda q: (plane, ALL, q)
        if name[1] == 'b':
            return third, 2, lambda q: (plane, my, q)
        return third, 1, lambda q: (plane, q, ALL)

    def ag_ref(name, off, rows):
        third, dim, where = ag_where(name)
        return kv.at[(*where(coord(dim, off)), pl.ds(*rows))]

    def ag_split(third):
        start, size = AG_ROWS[third]
        return (start, AG_HALF[third]), (start + AG_HALF[third], size - AG_HALF[third])

    def ag_push(name, kind, off, rows):
        n = AG_RINGS.index(name)
        ref = ag_ref(name, off, rows)
        push(ref, ref, ag_send.at[n, kind], ag_recv.at[n, kind], device(ag_where(name)[1], 1 if kind % 2 == 0 else -1))
        sends.append(lambda: (ag_ref(name, off, rows), ag_send.at[n, kind]))

    def direct(*names):
        for name in names:
            for kind in BOTH:
                ag_push(name, kind, 0, AG_ROWS[int(name[0])])

    def relay(*names):
        for name in names:
            third = int(name[0])
            for kind in BOTH:
                off = -1 if kind == 0 else 1
                landed(ag_ref(name, off, AG_ROWS[third]), ag_recv.at[AG_RINGS.index(name), kind])
                ag_push(name, 2 + kind, off, ag_split(third)[kind])

    def done(*names):
        for name in names:
            for kind in BOTH:
                landed(ag_ref(name, 2, ag_split(int(name[0]))[kind]), ag_recv.at[AG_RINGS.index(name), 2 + kind])

    def rs_where(name):
        if name in ('0z', '1z'):
            return lambda q: (q, my, mx)
        if name[:2] == '3x':
            row = coord(1, int(name[2]))
            return lambda q: (mz, row, q)
        if name == '3y':
            return lambda q: (mz, q, mx)
        if name == '4y':
            return lambda q: (mz, q, ALL)
        if name == '4x':
            return lambda q: (mz, my, q)
        if name[:2] == '2z':
            row = coord(1, int(name[2]))
            return lambda q: (q, row, ALL)
        plane = coord(0, int(name[2]))
        if name[:2] == '0x':
            row = coord(1, int(name[3]))
            return lambda q: (plane, row, q)
        return {'1y': lambda q: (plane, q, ALL), '0y': lambda q: (plane, q, mx), '1x': lambda q: (plane, my, q)}[name[:2]]

    def rs_split(part):
        start, size = RS_ROWS[part]
        return (start, RS_HALF[part]), (start + RS_HALF[part], size - RS_HALF[part])

    def rs_ref(name, q, rows):
        return dkv.at[(*rs_where(name)(q), pl.ds(*rows))]

    def rs_land(name, kind, sign):
        part, _, free = RS_RINGS[name]
        n = RS_NAMES.index(name)
        h = rs_split(part)
        lead = (ALL,) * free
        if kind == 0:
            return rs_bufs[2 * n].at[(sign, *lead, pl.ds(0, h[sign][1]))]
        rows = h[1 - sign] if kind == 1 else h[sign]
        return rs_bufs[2 * n + 1].at[(sign, *lead, pl.ds(rows[0] - RS_ROWS[part][0], rows[1]))]

    def rs_push(name, kind, sign, q, rows):
        n = RS_NAMES.index(name)
        push(rs_ref(name, q, rows), rs_land(name, kind, sign), rs_send.at[n, 2 * kind + sign],
             rs_recv.at[n, 2 * kind + sign], device(RS_RINGS[name][1], 1 if sign == 0 else -1))
        off = 2 if kind == 0 else 1 if sign == 0 else -1
        sends.append(lambda: (rs_ref(name, coord(RS_RINGS[name][1], off), rows), rs_send.at[n, 2 * kind + sign]))

    def rs_landed(name, kind, sign):
        landed(rs_land(name, kind, sign), rs_recv.at[RS_NAMES.index(name), 2 * kind + sign])

    def rs_add(name, q, rows, sources):
        free = RS_RINGS[name][2]
        where = rs_where(name)(q)

        def one(u, carry):
            sub = [lax.rem(u // SIDE ** (free - 1 - n), SIDE) for n in range(free)]
            left = iter(sub)
            idx = tuple(next(left) if w is ALL else w for w in where)
            total = dkv[(*idx, slice(rows[0], rows[0] + rows[1]), ALL)]
            for ref, offset in sources:
                total = total + ref[(*sub, slice(offset, offset + rows[1]), ALL)]
            dkv[(*idx, slice(rows[0], rows[0] + rows[1]), ALL)] = total
            return carry

        if free:
            lax.fori_loop(0, SIDE ** free, one, 0)
        else:
            one(0, 0)

    def rs_far(name, signs=BOTH):
        part, dim, _ = RS_RINGS[name]
        for sign in signs:
            rs_push(name, 0, sign, coord(dim, 2), rs_split(part)[sign])

    def rs_raw(name, signs=BOTH):
        part, dim, _ = RS_RINGS[name]
        for sign in signs:
            rs_push(name, 1, sign, coord(dim, 1 if sign == 0 else -1), rs_split(part)[1 - sign])

    def rs_mid(name, signs=BOTH):
        part, dim, _ = RS_RINGS[name]
        n = RS_NAMES.index(name)
        for sign in signs:
            rows = rs_split(part)[sign]
            q = coord(dim, 1 if sign == 0 else -1)
            rs_landed(name, 0, sign)
            rs_add(name, q, rows, [(rs_bufs[2 * n].at[sign], 0)])
            rs_push(name, 2, sign, q, rows)

    def rs_fin(name):
        part, dim, _ = RS_RINGS[name]
        n = RS_NAMES.index(name)
        for kind in (1, 2):
            for sign in BOTH:
                rs_landed(name, kind, sign)
        rs_add(name, me[dim], RS_ROWS[part], [(rs_bufs[2 * n + 1].at[0], 0), (rs_bufs[2 * n + 1].at[1], 0)])

    def each(f, *names):
        for name in names:
            f(name)

    def rs_start(name):
        rs_far(name)
        rs_raw(name)

    scale = HEAD_DIM ** -0.5
    c = scale * LOG2E

    def lanes_of(half):
        return pl.ds(pl.multiple_of(half * width, PIECE), width)

    def allowed(j0, second, half):
        row = lax.broadcasted_iota(jnp.int32, (512, 1), 0)
        b = row // PIECE
        kpiece = j0 + b + second * (127 - 2 * (j0 + b))
        kpos = kpiece * PIECE + lax.rem(row, PIECE)
        qpiece = rank + half * (127 - 2 * rank)
        qpos = qpiece * PIECE + lax.rem(lax.broadcasted_iota(jnp.int32, (1, width), 1), PIECE)
        return kpos <= qpos

    def scores(k, ql, mask=None):
        s = dot(k, qt_ref[:, ql])
        return s if mask is None else jnp.where(mask, s, LOWEST)

    def online(s, v, ql, mask=None):
        m_old = m_ref[:, ql]
        m_new = jnp.maximum(m_old, jnp.max(s, axis=0, keepdims=True))
        alpha = jnp.exp2((m_old - m_new) * c)
        p = jnp.exp2((s - m_new) * c)
        if mask is not None:
            p = jnp.where(mask, p, 0.0)
        m_ref[:, ql] = m_new
        l_ref[:, ql] = l_ref[:, ql] * alpha + jnp.sum(p, axis=0, keepdims=True)
        acc[:, ql] = acc[:, ql] * alpha + dot_ta(v, p.astype(BF))

    def bwd_tile(half, mask):
        ql = lanes_of(half)
        k = kt[...]
        p = jnp.exp2(dot(k, qt_ref[:, ql]) * c - m_ref[:, ql])
        if mask is not None:
            p = jnp.where(mask, p, 0.0)
        pb = p.astype(BF)
        ds = (pb.astype(F32) * (dot(vt[...], dot_ref[:, ql]) - delta[:, ql])).astype(BF)
        dqt[:, ql] += dot_ta(k, ds)
        return dot(ds, q_ref[ql, :]) * scale, dot(pb, do_ref[ql, :])

    def group_loop(zp, yp, body):
        here = zp * SIDE + yp
        mine = mz * SIDE + my
        mixed = here == mine
        high = here > mine
        count = jnp.where(mixed, 3, 2)

        def step(u, carry):
            second = jnp.logical_and(mixed, u == 2)
            half = jnp.where(jnp.logical_or(high, u == 2), 1, u)
            masked = jnp.logical_and(mixed, u != 1)

            @pl.when(high)
            def _():
                kt[...] = kv[zp, yp, pl.ds(2 * u, 2), KEYS, :].reshape(BLOCK, HEAD_DIM)
                vt[...] = kv[zp, yp, pl.ds(2 * u, 2), VALUES, :].reshape(BLOCK, HEAD_DIM)

            @pl.when(jnp.logical_and(jnp.logical_not(high), jnp.logical_not(second)))
            def _():
                kt[...] = kv[zp, yp, :, KEY_A, :].reshape(BLOCK, HEAD_DIM)
                vt[...] = kv[zp, yp, :, VAL_A, :].reshape(BLOCK, HEAD_DIM)

            @pl.when(second)
            def _():
                kt[...] = kv[zp, yp, :, KEY_B, :].reshape(BLOCK, HEAD_DIM)
                vt[...] = kv[zp, yp, :, VAL_B, :].reshape(BLOCK, HEAD_DIM)

            body(u, here * 4, second, high, half, masked)
            return carry

        lax.fori_loop(0, count, step, 0)

    def chunks(lo, hi):
        return [slice(n, n + 384) for n in range(lo, hi, 384)]

    def stream(work):
        held = [scores(k, ql) for k, _, ql in work[:1]]
        for n, (_, v, ql) in enumerate(work):
            if n + 1 < len(work):
                k, _, later = work[n + 1]
                held.append(scores(k, later))
            online(held.pop(0), v, ql)

    def fwd_group(zp, yp):
        here = zp * SIDE + yp
        mine = mz * SIDE + my

        @pl.when(here < mine)
        def _():
            k = kv[zp, yp, :, KEY_A, :].reshape(BLOCK, HEAD_DIM)
            v = kv[zp, yp, :, VAL_A, :].reshape(BLOCK, HEAD_DIM)
            stream([(k, v, ql) for ql in chunks(0, 2 * width)])

        @pl.when(here > mine)
        def _():
            pairs = (slice(0, 2), slice(2, 4))
            work = [(kv[zp, yp, pair, KEYS, :].reshape(BLOCK, HEAD_DIM), kv[zp, yp, pair, VALUES, :].reshape(BLOCK, HEAD_DIM))
                    for pair in pairs]
            stream([(k, v, ql) for k, v in work for ql in chunks(width, 2 * width)])

        def body(u, j0, second, high, half, masked):
            ql = lanes_of(half)
            mask = allowed(j0, jnp.where(second, 1, 0), half)
            online(scores(kt[...], ql, mask), vt[...], ql, mask)

        @pl.when(here == mine)
        def _():
            group_loop(zp, yp, body)

    def bwd_group(zp, yp):
        def first(dk, dv):
            none = jnp.zeros((SIDE, PIECE, HEAD_DIM), F32)
            dkv[zp, yp, :, KEY_A, :] = dk.reshape(SIDE, PIECE, HEAD_DIM)
            dkv[zp, yp, :, KEY_B, :] = none
            dkv[zp, yp, :, VAL_A, :] = dv.reshape(SIDE, PIECE, HEAD_DIM)
            dkv[zp, yp, :, VAL_B, :] = none

        def body(u, j0, second, high, half, masked):
            def keep(dk, dv):
                @pl.when(high)
                def _():
                    dkv[zp, yp, pl.ds(2 * u, 2), KEYS, :] = dk.reshape(2, 2 * PIECE, HEAD_DIM)
                    dkv[zp, yp, pl.ds(2 * u, 2), VALUES, :] = dv.reshape(2, 2 * PIECE, HEAD_DIM)

                @pl.when(jnp.logical_and(jnp.logical_not(high), u == 0))
                def _():
                    first(dk, dv)

                @pl.when(jnp.logical_and(jnp.logical_not(high), u != 0))
                def _():
                    dkv[zp, yp, :, KEY_A, :] += dk.reshape(SIDE, PIECE, HEAD_DIM)
                    dkv[zp, yp, :, VAL_A, :] += dv.reshape(SIDE, PIECE, HEAD_DIM)

            @pl.when(jnp.logical_not(masked))
            def _():
                keep(*bwd_tile(half, None))

            @pl.when(masked)
            def _():
                dk, dv = bwd_tile(half, allowed(j0, jnp.where(second, 1, 0), half))

                @pl.when(second)
                def _():
                    dkv[zp, yp, :, KEY_B, :] = dk.reshape(SIDE, PIECE, HEAD_DIM)
                    dkv[zp, yp, :, VAL_B, :] = dv.reshape(SIDE, PIECE, HEAD_DIM)

                @pl.when(jnp.logical_not(second))
                def _():
                    first(dk, dv)

        group_loop(zp, yp, body)

    def spiral(n):
        return n + n // 2 - 2 * (n // 3)

    def run(compute, reverse, events):
        def step(g, carry):
            for at, ops in events.items():
                @pl.when(g == at)
                def _():
                    for f, *args in ops:
                        f(*args)
            d, r = g // 4, lax.rem(g, 4)
            if reverse:
                d, r = 3 - d, 3 - r
            compute(lax.rem(mz + spiral(d), SIDE), lax.rem(my + spiral(r), SIDE))
            return carry

        lax.fori_loop(0, 16, step, 0)

    m_ref[...] = jnp.full(m_ref.shape, LOWEST, F32)
    l_ref[...] = jnp.zeros(l_ref.shape, F32)
    acc[...] = jnp.zeros(acc.shape, F32)
    loads['x'].wait()
    x_copy = remote(xs.at[core], xs.at[core], pair_send.at[2], pair_recv.at[2], partner)
    x_copy.start()
    loads['wk'].wait()
    loads['wv'].wait()

    def project_kv(slot):
        rows = xs[slot]
        lo = pl.multiple_of(slot * PIECE, PIECE)
        kv[*me, pl.ds(lo, PIECE), :] = dot(rows, wk[...]).astype(BF)
        kv[*me, pl.ds(256 + lo, PIECE), :] = dot(rows, wv[...]).astype(BF)

    def spread(rows, slot, flat, flat_t):
        for h in range(groups):
            block = rows[:, h * HEAD_DIM:(h + 1) * HEAD_DIM]
            lo = pl.multiple_of((slot * groups + h) * PIECE, PIECE)
            flat[pl.ds(lo, PIECE), :] = block
            flat_t[:, pl.ds(lo, PIECE)] = block.T

    def project_q(slot):
        spread(dot(xs[slot], wq[...]).astype(BF), slot, q_ref, qt_ref)

    def project_do(slot):
        spread(dot_tb(dys[slot], wo[...]).astype(BF), slot, do_ref, dot_ref)

    project_kv(core)
    landed(xs.at[1 - core], pair_recv.at[2])
    project_kv(1 - core)
    direct('0r0', '1b0', '2b0', '0b0', '2a', '0a', '1a')
    loads['dy'].wait()
    dy_copy = remote(dys.at[core], dys.at[core], pair_send.at[3], pair_recv.at[3], partner)
    dy_copy.start()
    loads['wq'].wait()
    project_q(core)
    relay('1b0', '0r0', '0b0', '2a', '2b0')
    direct('0r1', '0r3', '2b1', '2b3')
    project_q(1 - core)
    relay('0a', '1a')
    direct('0b1', '1b1', '0b3', '1b3')
    done('1b0')
    direct('1c0')
    done('0b0')
    direct('0r2')
    done('2a')
    direct('2b2', '2c0')
    done('0r0', '2b0')
    run(fwd_group, False, {
        1: [(relay, '0b1', '1b1', '0b3', '1b3'), (done, '0a', '1a'), (direct, '0b2', '1b2'),
            (relay, '0r1', '2b1', '0r3', '2b3', '2b2'), (direct, '2c1', '2c3'), (relay, '1c0'),
            (done, '0b1'), (direct, '0c1'), (done, '1b1'), (direct, '1c1'),
            (loads['wo'].wait,), (project_do, core), (done, '0r1', '2b1')],
        2: [(relay, '0r2'), (done, '2b3', '2b2'), (direct, '2c2'),
            (done, '0b3'), (direct, '0c3'), (done, '1b3'), (direct, '1c3'), (relay, '0b2', '1b2'), (done, '0r3')],
        3: [(relay, '2c0'), (done, '0r2', '1c0'),
            (landed, dys.at[1 - core], pair_recv.at[3]), (project_do, 1 - core), (relay, '0c1', '1c1')],
        4: [(relay, '2c1', '2c3', '2c2'), (done, '0b2', '1b2'), (direct, '0c2', '1c2'), (done, '0c1', '1c1')],
        5: [(relay, '0c3', '1c3')],
        7: [(relay, '0c2', '1c2')],
        8: [(done, '0c3', '1c3')],
        12: [(done, '0c2', '1c2', '2c0', '2c1', '2c2', '2c3')],
    })
    x_copy.wait_send()
    dy_copy.wait_send()

    l = l_ref[...]
    o = (acc[...] * (1.0 / l)).astype(BF)
    delta[...] = jnp.sum(dot_ref[...].astype(F32) * o.astype(F32), axis=0, keepdims=True)
    m_ref[...] = m_ref[...] * c + jnp.log(l) * LOG2E

    def to_rows(value_t):
        for s in range(2):
            for h in range(groups):
                lo = (s * groups + h) * PIECE
                rows_bf[s, :, h * HEAD_DIM:(h + 1) * HEAD_DIM] = value_t[:, lo:lo + PIECE].T

    to_rows(o)
    y_copy = remote(y_part.at[0], y_recv, pair_send.at[0], pair_recv.at[0], partner)

    dqt[...] = jnp.zeros(dqt.shape, F32)
    plan = collections.defaultdict(list)

    def at(time, rank_in_time, f, *args):
        plan[time].append((rank_in_time, len(plan[time]), (f, *args)))

    low, up = (1,), (0,)
    for p, o in enumerate(INWARD):
        for k, r in enumerate(INWARD):
            t = SIDE * p + k + 1
            sign = low if k == 1 else up
            side = low if p == 1 else up
            row = f'0x{o}{r}'
            at(t, 0, rs_start, row)
            at(t + 2, 1, rs_mid, row)
            at(t + 4, 2, rs_fin, row)
            if p == 0:
                at(t, 0, rs_far, f'2z{r}')
            elif p < 3:
                at(t, 0, rs_raw, f'2z{r}', side)
                at(t, 1, rs_mid, f'2z{r}', side)
            if k == 0:
                at(t, 0, rs_far, f'1y{o}')
                at(t + 4, 3, rs_far, f'0y{o}')
            elif k < 3:
                at(t, 0, rs_raw, f'1y{o}', sign)
                at(t + 1, 1, rs_mid, f'1y{o}', sign)
                at(t + 4, 3, rs_raw, f'0y{o}', sign)
                at(t + 5, 1, rs_mid, f'0y{o}', sign)
            else:
                at(t + 3, 2, rs_fin, f'1y{o}')
                at(t + 3, 3, rs_start, f'1x{o}')
                at(t + 5, 1, rs_mid, f'1x{o}')
                for late, name, last in ((6, '0z', f'0y{o}'), (7, '1z', f'1x{o}')):
                    at(t + late, 2, rs_fin, last)
                    if p == 0:
                        at(t + late, 3, rs_far, name)
                    elif p < 3:
                        at(t + late, 3, rs_raw, name, side)
                        at(21, 1, rs_mid, name, side)
                    else:
                        at(24, 2, rs_fin, name)
    for t, r, f, more in ((15, 2, rs_far, None), (17, 3, rs_raw, low), (18, 1, rs_raw, up), (19, 0, None, None)):
        at(t, 4, rs_fin, f'2z{r}')
        at(t, 5, rs_start, f'3x{r}')
        at(t + 2, 1, rs_mid, f'3x{r}')
        at(t + 3, 2, rs_fin, f'3x{r}')
        if f is None:
            at(20, 2, rs_fin, '4y')
            at(20, 2, rs_start, '4x')
            at(21, 1, rs_mid, '4x')
        else:
            for start, name, rank_in_time in ((t, '4y', 5), (t + 3, '3y', 2)):
                if more is None:
                    at(start, rank_in_time, f, name)
                else:
                    at(start, rank_in_time, f, name, more)
                    at(start + 1, 0, rs_mid, name, more)
    for name in ('3y', '4x'):
        at(23, 2, rs_fin, name)
    plan = {time: [op for _, _, op in sorted(ops, key=lambda e: e[:2])] for time, ops in sorted(plan.items())}
    run(bwd_group, True, {time: ops for time, ops in plan.items() if time < 16})

    def dx_start():
        y_part[0] = dot(rows_bf[1 - core], wo[...])
        y_copy.start()
        y_part[1] = dot(rows_bf[core], wo[...])
        to_rows((dqt[...] * scale).astype(BF))
        dx_part[0] = dot_tb(rows_bf[1 - core], wq[...])

    for time, ops in plan.items():
        if time >= 16:
            for f, *args in ops:
                f(*args)
            if time == 16:
                dx_start()
            if time == 17:
                dx_part[1] = dot_tb(rows_bf[core], wq[...])
                y_copy.wait_recv()
                y_out[...] = (y_part[1] + y_recv[...]).astype(BF)

    dk_own = dkv[*me, KEYS, :].astype(BF)
    dv_own = dkv[*me, VALUES, :].astype(BF)
    kt[0:256, :] = dk_own
    vt[0:256, :] = dv_own

    def add_kv(slot, side):
        rows = pl.ds(pl.multiple_of(side * PIECE, PIECE), PIECE)
        dx_part[slot] = dx_part[slot] + dot_tb(kt[rows, :], wk[...]) + dot_tb(vt[rows, :], wv[...])

    add_kv(0, 1 - core)
    dx_copy = remote(dx_part.at[0], dx_recv, pair_send.at[1], pair_recv.at[1], partner)
    dx_copy.start()
    add_kv(1, core)
    for sent in sends:
        landed(*sent())
    y_copy.wait_send()
    dx_copy.wait_recv()
    dx_out[...] = (dx_part[1] + dx_recv[...]).astype(BF)
    dx_copy.wait_send()


def attention(x_blk, dy_blk, w_query, w_key, w_value, w_out, groups):
    lanes = 2 * groups * PIECE
    dim = w_query.shape[0]
    vmem = pl.BlockSpec(memory_space=pltpu.VMEM)
    anywhere = pl.BlockSpec(memory_space=pl.ANY)
    weights = (w_query, w_key, w_value, w_out)
    return pl.pallas_call(
        functools.partial(kernel, groups),
        out_shape=(jax.ShapeDtypeStruct((PIECE, dim), BF),) * 2,
        in_specs=[anywhere] * 6,
        out_specs=(vmem,) * 2,
        scratch_shapes=[
            pltpu.VMEM((2, *x_blk.shape), BF), pltpu.VMEM((2, *x_blk.shape), BF),
            *[pltpu.VMEM(shape, BF) for shape in ((HEAD_DIM, lanes), (lanes, HEAD_DIM)) * 2],
            pltpu.VMEM((*TORUS, BLOCK, HEAD_DIM), BF),
            pltpu.VMEM((*TORUS, BLOCK, HEAD_DIM), F32),
            pltpu.VMEM((1, lanes), F32), pltpu.VMEM((1, lanes), F32),
            pltpu.VMEM((HEAD_DIM, lanes), F32), pltpu.VMEM((1, lanes), F32),
            pltpu.VMEM((BLOCK, HEAD_DIM), BF), pltpu.VMEM((BLOCK, HEAD_DIM), BF),
            *[pltpu.VMEM(w.shape, BF) for w in weights],
            pltpu.VMEM((2, PIECE, groups * HEAD_DIM), BF),
            pltpu.VMEM((2, PIECE, dim), F32), pltpu.VMEM((PIECE, dim), F32),
            pltpu.VMEM((2, PIECE, dim), F32), pltpu.VMEM((PIECE, dim), F32),
            pltpu.SemaphoreType.DMA((6,)),
            pltpu.SemaphoreType.DMA((4,)), pltpu.SemaphoreType.DMA((4,)),
            pltpu.SemaphoreType.DMA((len(AG_RINGS), 4)), pltpu.SemaphoreType.DMA((len(AG_RINGS), 4)),
            pltpu.SemaphoreType.DMA((len(RS_NAMES), 6)), pltpu.SemaphoreType.DMA((len(RS_NAMES), 6)),
            *rs_scratch(),
        ],
        compiler_params=pltpu.CompilerParams(collective_id=0, has_side_effects=True, vmem_limit_bytes=67043328),
        name='attention',
    )(x_blk, dy_blk, *weights)


def handover(y, dx):
    def body(y_in, dx_in, y_end, dx_end):
        y_end[...] = y_in[...]
        dx_end[...] = dx_in[...]

    vmem = pl.BlockSpec(memory_space=pltpu.VMEM)
    shape = jax.ShapeDtypeStruct(y.shape, y.dtype)
    return pl.pallas_call(body, out_shape=(shape, shape), in_specs=[vmem] * 2, out_specs=(vmem,) * 2, name='handover')(y, dx)


def solution(mesh):
    row_spec = P(('dp', 'cp', 'tp'), None)

    def local_step(x_blk, dy_blk, w_query, w_key, w_value, w_out):
        groups = w_query.shape[1] // HEAD_DIM
        return handover(*attention(x_blk, dy_blk, w_query, w_key, w_value, w_out, groups))

    return jax.shard_map(local_step, mesh=mesh,
                         in_specs=(row_spec, row_spec, P(None, 'tp'), P(None, 'tp'), P(None, 'tp'), P('tp', None)),
                         out_specs=(row_spec, row_spec), check_vma=False)
```
